32 devices in a mesh: tau: 4 (over x, core), tile: 8 (over z, y).
Axes of the slice: x: 2, y: 2, z: 4, core: 2. Of those that a mesh axis runs over, the one named last changes fastest.
Arguments:
- occupied: bfloat16 [4, 1024, 128, 128], P('tau', 'tile'), may hold values from -6 to 6
- virtual: bfloat16 [4, 1024, 128, 128], P('tau', 'tile'), may hold values from -0.125 to 0.125
- cos_weights: float32 [4, 4], replicated, may hold values from -1 to 1
- pair_occ: int32 [1536, 16], P('tile'), may hold values from 0 to 127
- pair_virt: int32 [1536, 16], P('tile'), may hold values from 0 to 127
- partial_target_tile: int32 [1536], P('tile'), may hold values from 0 to 255, as said below
Outputs:
- spectrum: float32 [4, 256, 128, 128], P(None, 'tile', 'tau')
The draws below stay inside these ranges and needn't reach their ends.
Inputs may be any that keep to these rules, and one draw needn't show every extreme that they name: `partial_target_tile`: within each aligned block of 192 entries, no owner (values d * 32 to (d + 1) * 32 - 1 for owner d) is named more than 48 times; one owner is named exactly 48 times in every block.
All inputs are finite; a program needn't handle non-finite values.
Results may differ from the reference program's by a relative error of at most 0.0003.
Values sent between devices are 32-bit elements; how exact they have to be, the bound alone decides.
A program may use at most 192 MiB of HBM per device.

```python
import math
import jax
import jax.numpy as jnp
from jax import lax

TILE = 128
TERMS = 16
NFREQ = 4
SLOT_DEV = 128
PART_DEV = 192
CHI_DEV = 32
NTAU = 4
NOCC = 1024
NPART = 1536
NCHI = 256
CAP = 48


def draw_partial_target_tile(key, part):
    owners = NPART // PART_DEV
    first, second, third, fourth = jax.random.split(jax.random.fold_in(key, 7), 4)
    complete_holder = jax.random.randint(first, (), 0, owners)
    owner_preference = jax.random.randint(second, (owners, owners), 0, 1 << 19)
    random_perturbation = jax.random.randint(third, (owners, owners, CAP), 0, 1 << 19)
    holder_indices = jnp.arange(owners, dtype=jnp.int32)
    extra_credit = jnp.where(holder_indices == complete_holder, 1 << 20, 0).astype(jnp.int32)
    ranking_value = owner_preference[:, :, None] + random_perturbation + extra_credit[None, :, None]
    places = jnp.arange(owners * CAP, dtype=jnp.int32).reshape(owners, CAP)
    ranking_value = ranking_value * (owners * CAP) + places[None]
    flat = ranking_value.reshape(owners, owners * CAP)
    _, chosen = lax.top_k(flat, PART_DEV)
    owner = (chosen // CAP).astype(jnp.int32)
    within = jax.random.randint(fourth, (owners, PART_DEV), 0, CHI_DEV)
    return (owner * CHI_DEV + within).reshape(-1).astype(jnp.int32)


def touch_ends(drawn, stream_key, low, largest):
    longest = drawn.shape.index(max(drawn.shape))
    spots = []
    for shift in (0, 1):
        where = [jax.random.randint(jax.random.fold_in(stream_key, axis), (), 0, length) for axis, length in enumerate(drawn.shape)]
        where[longest] = (where[longest] + shift) % drawn.shape[longest]
        spots.append(tuple(where))
    return drawn.at[spots[0]].set(low).at[spots[1]].set(largest)


def level_of(rng, dims, pieces, least, largest):
    factor_of = 1.0
    for position, parts in pieces:
        draws = jax.random.uniform(jax.random.fold_in(jax.random.fold_in(rng, 6), position), (parts,), jnp.float32, least / len(pieces), largest / len(pieces))
        factor_of = factor_of * jnp.repeat(jnp.exp(draws), dims[position] // parts).reshape((-1,) + (1,) * (len(dims) - 1 - position))
    return factor_of


def noise(rng, dims, width, reach, cuts=(), held_as=jnp.bfloat16):
    array = width * jax.random.normal(rng, dims, jnp.float32)
    if cuts:
        array = array * level_of(rng, dims, cuts, -0.22, 0.18)
    return jnp.clip(array, -reach, reach).astype(held_as)


def setup_inputs(seed: int = 0) -> dict:
    splits = jax.random.split(jax.random.key(seed), 7)
    return {
        "occupied": noise(splits[0], (NTAU, NOCC, TILE, TILE), 1.0, 6.0, ((0, 4), (1, 8))),
        "virtual": noise(splits[1], (NTAU, NOCC, TILE, TILE), (TILE * TERMS) ** -0.5, 0.125, ((0, 4), (1, 8))),
        "cos_weights": jnp.clip(jax.random.uniform(splits[2], (NFREQ, NTAU), jnp.float32, -1.0, 1.0), -1.0, 1.0),
        "pair_occ": touch_ends(jax.random.randint(splits[3], (NPART, TERMS), 0, SLOT_DEV), jax.random.fold_in(splits[3], 1), 0, SLOT_DEV - 1).astype(jnp.int32),
        "pair_virt": touch_ends(jax.random.randint(splits[4], (NPART, TERMS), 0, SLOT_DEV), jax.random.fold_in(splits[4], 1), 0, SLOT_DEV - 1).astype(jnp.int32),
        "partial_target_tile": draw_partial_target_tile(jax.random.fold_in(splits[6], 71), 0),
    }


def reference(occupied, virtual, cos_weights, pair_occ, pair_virt, partial_target_tile):
    owner_base = (jnp.arange(NPART, dtype=jnp.int32) // PART_DEV) * SLOT_DEV
    occ_global = (pair_occ + owner_base[:, None]).astype(jnp.int32)
    virt_global = (pair_virt + owner_base[:, None]).astype(jnp.int32)
    group = math.gcd(NPART, 16)
    count = NPART // group
    occ_blocks = occ_global.reshape(count, group, TERMS)
    virt_blocks = virt_global.reshape(count, group, TERMS)
    dest_blocks = partial_target_tile.astype(jnp.int32).reshape(count, group)

    def time_step(spectrum, step_index):
        occ_now = lax.dynamic_index_in_dim(occupied, step_index, 0, keepdims=False)
        virt_now = lax.dynamic_index_in_dim(virtual, step_index, 0, keepdims=False)

        def add_block(chi_time, items):
            left = jnp.take(occ_now, items[0], axis=0).astype(jnp.float32)
            right = jnp.take(virt_now, items[1], axis=0).astype(jnp.float32)
            product = jnp.einsum("bjrk,bjkc->brc", left, right, precision=lax.Precision.HIGHEST)
            return chi_time.at[items[2]].add(product), None

        chi_time, _ = lax.scan(add_block, jnp.zeros((NCHI, TILE, TILE), jnp.float32),
                               (occ_blocks, virt_blocks, dest_blocks))
        weights = lax.dynamic_index_in_dim(cos_weights, step_index, 1, keepdims=False)
        return spectrum + weights[:, None, None, None] * chi_time[None], None

    spectrum, _ = lax.scan(time_step, jnp.zeros((NFREQ, NCHI, TILE, TILE), jnp.float32),
                           jnp.arange(NTAU, dtype=jnp.int32))
    return spectrum
```

```python
import functools
import math

import jax
import jax.numpy as jnp
from jax import lax
from jax.experimental import pallas as pl
from jax.experimental.pallas import tpu as pltpu
from jax.sharding import PartitionSpec as P

CHI_DEV = 32
UNIT = 2
Z_FIRST = 3 / 16
BUDGET = 46 * 1024 * 1024
MESH = pl.DeviceIdType.MESH


def products_kernel(first, terms, chi_dev, occ_idx, virt_idx, target, occ, virt, out):
    owners, units, groups, each, rows, width = out.shape
    span = units * each
    count = target.shape[0]

    @pl.loop(0, owners)
    def _(d):
        out[d] = jnp.zeros(out.shape[1:], out.dtype)

    unroll = math.gcd(count, 4) if span == chi_dev else 1

    @pl.loop(0, count, unroll=unroll)
    def _(p):
        tile = target[p]
        owner = tile // chi_dev
        place = tile - owner * chi_dev - first

        def add():
            unit = place // each
            left = [occ[occ_idx[j, p]] for j in range(terms)]
            right = [virt[virt_idx[j, p]] for j in range(terms)]
            acc = jnp.dot(
                jnp.concatenate(left, axis=1),
                jnp.concatenate(right, axis=0),
                preferred_element_type=jnp.float32,
            )
            for g in range(groups):
                out[owner, unit, g, place - unit * each] += acc[g * rows : (g + 1) * rows]

        if span == chi_dev:
            add()
        else:
            pl.when((place >= 0) & (place < span))(add)


def products(occ, virt, occ_idx, virt_idx, target, first, span, each, owners, groups):
    terms = occ_idx.shape[1]
    size = occ.shape[1]
    smem = pl.BlockSpec(memory_space=pltpu.SMEM)
    vmem = pl.BlockSpec(memory_space=pltpu.VMEM)
    return pl.pallas_call(
        functools.partial(products_kernel, first, terms, CHI_DEV),
        out_shape=jax.ShapeDtypeStruct(
            (owners, span // each, groups, each, size // groups, size), jnp.float32
        ),
        in_specs=[smem, smem, smem, vmem, vmem],
        out_specs=vmem,
        compiler_params=pltpu.CompilerParams(vmem_limit_bytes=56 * 1024 * 1024),
        cost_estimate=pl.CostEstimate(
            flops=2 * target.shape[0] * terms * size**3 * span // CHI_DEV,
            bytes_accessed=occ.size * 4 + owners * span * size * size * 4,
            transcendentals=0,
        ),
    )(occ_idx.T, virt_idx.T, target, occ, virt)


def line_slots(n):
    if n == 1:
        return 0
    return 1 if n == 2 else 2 * (n - 1)


class Line:
    def __init__(self, n, place, device, own, slots, send_sem, recv_sem, hold=None):
        self.hold = hold
        self.n, self.place, self.device = n, place, device
        self.own, self.slots, self.send_sem, self.recv_sem = own, slots, send_sem, recv_sem

    def slot(self, right, d):
        if right:
            return d - 1
        return d if self.n == 2 else self.n - 1 + d

    def copy(self, right, u, d, src, back=False):
        s = self.slot(right, d)
        k = u * line_slots(self.n) + s
        return pltpu.make_async_remote_copy(
            src_ref=src,
            dst_ref=self.slots.at[s, u],
            send_sem=self.send_sem.at[k],
            recv_sem=self.recv_sem.at[k],
            device_id={"tile": self.device(1 if right != back else -1)},
            device_id_type=MESH,
        )

    def routes(self):
        for right in (True, False):
            for d in range(self.n - 1, 0, -1) if right else range(self.n - 1):
                yield right, d

    def launch(self, u):
        for right, d in self.routes():
            @pl.when(self.place == (0 if right else self.n - 1))
            def _():
                self.copy(right, u, d, self.own(d, u)).start()

    def merge(self, u):
        if self.n == 2:
            return
        for right, d in self.routes():
            inner = (self.place > 0) & (self.place < d) if right else (
                (self.place < self.n - 1) & (self.place > d))

            @pl.when(inner)
            def _():
                here = self.slots.at[self.slot(right, d), u]
                copy = self.copy(right, u, d, here)
                copy.wait_recv()
                own = self.own(d, u)
                if self.hold is not None:
                    buffer, sem = self.hold
                    fetch = pltpu.make_async_copy(own, buffer, sem)
                    fetch.start()
                    fetch.wait()
                    own = buffer
                here[...] += own[...]
                copy.start()

    def final(self, u, into):
        for right in (True, False):
            @pl.when(self.place > 0 if right else self.place < self.n - 1)
            def _():
                k = self.slot(right, self.place)
                here = self.slots.at[k, u]
                self.copy(right, u, self.place, here, back=True).wait_recv()
                into[...] += here[...]

    def drain(self, u):
        for right, d in self.routes():
            @pl.when(self.place < d if right else self.place > d)
            def _():
                self.copy(right, u, d, self.slots.at[self.slot(right, d), u]).wait_send()


def scatter_kernel(ny, nz, groups, weights, dense, out, mine, y_slots, z_slots, times,
                   load_sem, y_send, y_recv, z_send, z_recv, t_send, t_recv, hold, hold_sem,
                   both, z2_slots, y2_slots, both_sem, z2_send, z2_recv, y2_send, y2_recv):
    tau = lax.axis_index("tau")
    tile = lax.axis_index("tile")
    z, y = tile // ny, tile % ny
    units = mine.shape[0]
    lead = both.shape[0]
    last = units - lead
    each = mine.shape[3]
    freqs = out.shape[0]

    y_line = Line(ny, y, lambda step: tile + step, lambda d, u: dense.at[:, d, u],
                  y_slots, y_send, y_recv, (hold, hold_sem))
    z_line = Line(nz, z, lambda step: tile + step * ny, lambda d, u: mine.at[u, d],
                  z_slots, z_send, z_recv)

    z2_line = Line(nz, z, z_line.device, lambda d, u: both.at[u, d], z2_slots, z2_send, z2_recv)
    y2_line = Line(ny, y, y_line.device, lambda d, u: both.at[u, z, d], y2_slots, y2_send, y2_recv)

    barrier = pltpu.get_barrier_semaphore()
    for step in range(1, groups):
        pl.semaphore_signal(barrier, inc=1, device_id={"tau": (tau + step) % groups},
                            device_id_type=MESH)
    for step in range(1, ny):
        pl.semaphore_signal(barrier, inc=1, device_id={"tile": z * ny + (y + step) % ny},
                            device_id_type=MESH)
    for step in range(1, nz):
        pl.semaphore_signal(barrier, inc=1, device_id={"tile": (z + step) % nz * ny + y},
                            device_id_type=MESH)
    pl.semaphore_wait(barrier, groups - 1 + ny - 1 + nz - 1)

    def load(u):
        return pltpu.make_async_copy(dense.at[:, y, u], mine.at[u], load_sem.at[u])

    def swap(u, step):
        other = (tau + step) % groups
        return pltpu.make_async_remote_copy(
            src_ref=mine.at[u, z, other],
            dst_ref=times.at[u, tau],
            send_sem=t_send.at[u * groups + step],
            recv_sem=t_recv.at[u * groups + tau],
            device_id={"tau": other},
            device_id_type=MESH,
        )

    def arrived(u, source):
        return pltpu.make_async_remote_copy(
            src_ref=mine.at[u, z, 0],
            dst_ref=times.at[u, source],
            send_sem=t_send.at[u * groups],
            recv_sem=t_recv.at[u * groups + source],
            device_id={"tau": source},
            device_id_type=MESH,
        )

    def whole(w):
        return pltpu.make_async_copy(dense.at[:, :, last + w], both.at[w], both_sem.at[w])

    @pl.loop(0, lead)
    def _(w):
        whole(w).start()

    @pl.loop(0, last)
    def _(u):
        y_line.launch(u)
        load(u).start()

    @pl.loop(0, lead)
    def _(w):
        whole(w).wait()
        z2_line.launch(w)

    @pl.loop(0, lead)
    def _(w):
        z2_line.merge(w)

    @pl.loop(0, units + 2)
    def _(t):
        @pl.when(t < last)
        def _():
            load(t).wait()
            y_line.merge(t)
            y_line.final(t, mine.at[t])
            z_line.launch(t)

        @pl.when(t < lead)
        def _():
            z2_line.final(t, both.at[t, z])
            y2_line.launch(t)

        @pl.when((t >= 1) & (t < last + 1))
        def _():
            u = t - 1
            z_line.merge(u)
            z_line.final(u, mine.at[u, z])

        @pl.when((t >= last + 1) & (t < units + 1))
        def _():
            w = t - 1 - last
            y2_line.merge(w)
            mine[t - 1, z] = both[w, z, y]
            y2_line.final(w, mine.at[t - 1, z])

        @pl.when((t >= 1) & (t < units + 1))
        def _():
            u = t - 1
            for step in range(1, groups):
                swap(u, step).start()
            times[u, tau] = mine[u, z, tau]

        @pl.when(t >= 2)
        def _():
            u = t - 2
            for step in range(1, groups):
                arrived(u, (tau + step) % groups).wait_recv()
            for e in range(each):
                for k in range(freqs):
                    total = weights[k, 0] * times[u, 0, e]
                    for s in range(1, groups):
                        total += weights[k, s] * times[u, s, e]
                    out[k, u * each + e] = total

    @pl.loop(0, lead)
    def _(w):
        z2_line.drain(w)
        y2_line.drain(w)

    @pl.loop(0, last)
    def _(u):
        y_line.drain(u)
        z_line.drain(u)

    @pl.loop(0, units)
    def _(u):
        for step in range(1, groups):
            swap(u, step).wait_send()


def scatter(dense, weights, ny, nz, groups):
    owners, units, _, each, rows, width = dense.shape
    freqs = weights.shape[0]
    block = (groups, each, rows, width)
    lead = max(1, int(units * Z_FIRST))
    ys, zs = max(line_slots(ny), 1), max(line_slots(nz), 1)
    dma = pltpu.SemaphoreType.DMA
    return pl.pallas_call(
        functools.partial(scatter_kernel, ny, nz, groups),
        out_shape=jax.ShapeDtypeStruct((freqs, units * each, rows, width), jnp.float32),
        in_specs=[pl.BlockSpec(memory_space=pltpu.SMEM), pl.BlockSpec(memory_space=pl.ANY)],
        out_specs=pl.BlockSpec(memory_space=pltpu.VMEM),
        scratch_shapes=[
            pltpu.VMEM((units, nz) + block, jnp.float32),
            pltpu.VMEM((ys, units, nz) + block, jnp.float32),
            pltpu.VMEM((zs, units) + block, jnp.float32),
            pltpu.VMEM((units, groups, each, rows, width), jnp.float32),
            dma((units,)),
            dma((units * ys,)),
            dma((units * ys,)),
            dma((units * zs,)),
            dma((units * zs,)),
            dma((units * groups,)),
            dma((units * groups,)),
            pltpu.VMEM((nz,) + block if ny > 2 else (8, 128), jnp.float32),
            dma,
            pltpu.VMEM((lead, nz, ny) + block, jnp.float32),
            pltpu.VMEM((zs, lead, ny) + block, jnp.float32),
            pltpu.VMEM((ys, lead) + block, jnp.float32),
            dma((lead,)),
            dma((lead * zs,)),
            dma((lead * zs,)),
            dma((lead * ys,)),
            dma((lead * ys,)),
        ],
        compiler_params=pltpu.CompilerParams(
            collective_id=0, has_side_effects=True, vmem_limit_bytes=58 * 1024 * 1024),
    )(weights, dense.reshape((nz, ny) + dense.shape[1:]))


def far_first(nz, z, k):
    flip = z // (nz // 2)
    m = z + flip * (nz - 1 - 2 * z)
    ends = nz - 1 - k
    inner = (1 - k % 2) * (nz - 1 - k // 2) + (k % 2) * (k // 2)
    e = (1 - m) * ends + m * inner
    return e + flip * (nz - 1 - 2 * e)


def fused_kernel(nz, groups, terms, cap, weights, order, keep, slot, occ_idx, virt_idx, occ, virt,
                 out, packed, y_out, y_in, z_right, z_left, lead_own, z2_right, z2_left, y2_in,
                 times, y_send, y_recv, z_send, zr_recv, zl_recv, z2_send, z2r_recv, z2l_recv,
                 y2_send, y2_recv, t_send, t_recv):
    tau = lax.axis_index("tau")
    tile = lax.axis_index("tile")
    ny = 2
    z, y = tile // ny, tile % ny
    other_y = 1 - y
    lead = lead_own.shape[0]
    units = y_out.shape[1]
    each, rows = y_out.shape[3], y_out.shape[4]
    span = (units + lead) * each
    owners = nz * ny
    count = order.shape[0]
    freqs = out.shape[0]

    def dest(k):
        return far_first(nz, z, k)

    def remote(src, dst, send, recv, device):
        return pltpu.make_async_remote_copy(
            src_ref=src, dst_ref=dst, send_sem=send, recv_sem=recv,
            device_id=device, device_id_type=MESH)

    def y_copy(d, u):
        k = d * units + u
        return remote(y_out.at[d, u], y_in.at[d, u], y_send.at[k], y_recv.at[k],
                      {"tile": z * ny + other_y})

    def z_copy(right, d, u, src, back=False):
        if right:
            k = (d - 1) * units + u
            dst, recv = z_right.at[d - 1, u], zr_recv.at[k]
        else:
            k = d * units + u
            dst, recv = z_left.at[d, u], zl_recv.at[k]
        return remote(src, dst, z_send.at[d * units + u], recv,
                      {"tile": tile + (ny if right != back else -ny)})

    def z2_copy(right, d, yy, w, src, back=False):
        k = (d * ny + yy) * lead + w
        if right:
            dst, recv = z2_right.at[d - 1, yy, w], z2r_recv.at[k - ny * lead]
        else:
            dst, recv = z2_left.at[d, yy, w], z2l_recv.at[k]
        return remote(src, dst, z2_send.at[k], recv,
                      {"tile": tile + (ny if right != back else -ny)})

    def y2_copy(w):
        return remote(lead_own.at[w, z, other_y], y2_in.at[w], y2_send.at[w], y2_recv.at[w],
                      {"tile": z * ny + other_y})

    def swap(src, u, step):
        other = (tau + step) % groups
        return remote(src.at[other], times.at[u, tau], t_send.at[u * groups + step],
                      t_recv.at[u * groups + tau], {"tau": other})

    def arrived(u, source):
        return remote(times.at[u, tau], times.at[u, source], t_send.at[u * groups],
                      t_recv.at[u * groups + source], {"tau": source})

    barrier = pltpu.get_barrier_semaphore()
    for step in range(1, groups):
        pl.semaphore_signal(barrier, inc=1, device_id={"tau": (tau + step) % groups},
                            device_id_type=MESH)
    pl.semaphore_signal(barrier, inc=1, device_id={"tile": z * ny + other_y}, device_id_type=MESH)
    for step in range(1, nz):
        pl.semaphore_signal(barrier, inc=1, device_id={"tile": (z + step) % nz * ny + y},
                            device_id_type=MESH)
    pl.semaphore_wait(barrier, groups - 1 + ny - 1 + nz - 1)

    packed[0] = jnp.zeros(packed.shape[1:], packed.dtype)

    def product(s):
        p = order[s]
        left = [occ[occ_idx[j, p]] for j in range(terms)]
        right = [virt[virt_idx[j, p]] for j in range(terms)]
        acc = jnp.dot(
            jnp.concatenate(left, axis=1),
            jnp.concatenate(right, axis=0),
            preferred_element_type=jnp.float32,
        )
        packed[s + 1] = acc + keep[s] * packed[s]

    def fill(rank, u, ref, add):
        for e in range(each):
            part = packed[slot[rank * span + u * each + e]]
            for g in range(groups):
                piece = part[g * rows:(g + 1) * rows]
                if add:
                    ref[g, e] += piece
                else:
                    ref[g, e] = piece

    def ready(rank):
        d = dest(rank // 2)
        yy = y if rank % 2 else other_y
        if rank % 2 == 0:
            @pl.loop(0, units)
            def _(u):
                fill(rank, u, y_out.at[d, u], False)
                y_copy(d, u).start()

        @pl.loop(0, lead)
        def _(w):
            own = lead_own.at[w, d, yy]
            fill(rank, units + w, own, False)

            @pl.when((z == 0) & (d > z))
            def _():
                z2_copy(True, d, yy, w, own).start()

            @pl.when((z == nz - 1) & (d < z))
            def _():
                z2_copy(False, d, yy, w, own).start()

    def y_stage(i):
        k, u = i // units, i % units
        d = dest(k)
        here = y_in.at[d, u]
        y_copy(d, u).wait_recv()
        fill(2 * k + 1, u, here, True)

        @pl.when((z == 0) & (d > z))
        def _():
            z_copy(True, d, u, here).start()

        @pl.when((z == nz - 1) & (d < z))
        def _():
            z_copy(False, d, u, here).start()

    def z_stage(i):
        k, u = i // units, i % units
        d = dest(k)
        own = y_in.at[d, u]

        @pl.when((z > 0) & (d > z))
        def _():
            here = z_right.at[d - 1, u]
            copy = z_copy(True, d, u, here)
            copy.wait_recv()
            here[...] += own[...]
            copy.start()

        @pl.when((z < nz - 1) & (d < z))
        def _():
            here = z_left.at[d, u]
            copy = z_copy(False, d, u, here)
            copy.wait_recv()
            here[...] += own[...]
            copy.start()

        @pl.when((d == z) & (z > 0))
        def _():
            here = z_right.at[z - 1, u]
            z_copy(True, z, u, here, True).wait_recv()
            own[...] += here[...]

        @pl.when((d == z) & (z < nz - 1))
        def _():
            here = z_left.at[z, u]
            z_copy(False, z, u, here, True).wait_recv()
            own[...] += here[...]

        @pl.when(d == z)
        def _():
            for step in range(1, groups):
                swap(own, u, step).start()
            times[u, tau] = own[tau]

    def lead_stage(j):
        rank, w = j // lead, j % lead
        d = dest(rank // 2)
        yy = y + (1 - rank % 2) * (1 - 2 * y)
        own = lead_own.at[w, d, yy]

        @pl.when((z > 0) & (d > z))
        def _():
            here = z2_right.at[d - 1, yy, w]
            copy = z2_copy(True, d, yy, w, here)
            copy.wait_recv()
            here[...] += own[...]
            copy.start()

        @pl.when((z < nz - 1) & (d < z))
        def _():
            here = z2_left.at[d, yy, w]
            copy = z2_copy(False, d, yy, w, here)
            copy.wait_recv()
            here[...] += own[...]
            copy.start()

        @pl.when((d == z) & (z > 0))
        def _():
            here = z2_right.at[z - 1, yy, w]
            z2_copy(True, z, yy, w, here, True).wait_recv()
            own[...] += here[...]

        @pl.when((d == z) & (z < nz - 1))
        def _():
            here = z2_left.at[z, yy, w]
            z2_copy(False, z, yy, w, here, True).wait_recv()
            own[...] += here[...]

        @pl.when((d == z) & (rank % 2 == 0))
        def _():
            y2_copy(w).start()

    def cross_stage(w):
        own = lead_own.at[w, z, y]
        y2_copy(w).wait_recv()
        own[...] += y2_in[w]
        for step in range(1, groups):
            swap(own, units + w, step).start()
        times[units + w, tau] = own[tau]

    def out_stage(u):
        for step in range(1, groups):
            arrived(u, (tau + step) % groups).wait_recv()
        for e in range(each):
            for k in range(freqs):
                total = weights[k, 0] * times[u, 0, e]
                for s in range(1, groups):
                    total += weights[k, s] * times[u, s, e]
                out[k, u * each + e] = total

    early = 0
    phases = -(-count // cap)
    for phase in range(phases):
        @pl.loop(phase * cap, min(count, (phase + 1) * cap), unroll=2)
        def _(s):
            product(s)

        for rank in range(phase, phase + 1 if phase < phases - 1 else owners):
            ready(rank)
        upto = early
        if 1 <= phase < phases - 1:
            upto = early + 2 * phase

            @pl.loop(early, upto)
            def _(i):
                y_stage(i)
        early = upto

    items = nz * units
    hold = 2
    own_first = items - units + early

    @pl.loop(early, items + early + lead + hold)
    def _(t):
        @pl.when(t < items)
        def _():
            y_stage(t)

        @pl.when(t - early < owners * lead)
        def _():
            lead_stage(t - early)

        @pl.when(t - early < items)
        def _():
            z_stage(t - early)

        @pl.when((t >= items + early) & (t < items + early + lead))
        def _():
            cross_stage(t - items - early)

        @pl.when(t >= own_first + hold)
        def _():
            out_stage(t - own_first - hold)

    @pl.loop(0, units)
    def _(u):
        @pl.loop(0, nz)
        def _(d):
            y_copy(d, u).wait_send()

            @pl.when(d > z)
            def _():
                z_copy(True, d, u, y_in.at[d, u]).wait_send()

            @pl.when(d < z)
            def _():
                z_copy(False, d, u, y_in.at[d, u]).wait_send()

        for step in range(1, groups):
            swap(y_in.at[z, u], u, step).wait_send()

    @pl.loop(0, lead)
    def _(w):
        @pl.loop(0, nz)
        def _(d):
            for yy in range(ny):
                @pl.when(d > z)
                def _():
                    z2_copy(True, d, yy, w, lead_own.at[w, d, yy]).wait_send()

                @pl.when(d < z)
                def _():
                    z2_copy(False, d, yy, w, lead_own.at[w, d, yy]).wait_send()

        y2_copy(w).wait_send()
        for step in range(1, groups):
            swap(lead_own.at[w, z, y], units + w, step).wait_send()


def slot_tables(target, nz, span):
    ny = 2
    tile = lax.axis_index("tile")
    z, y = tile // ny, tile % ny
    owner = target // span
    zd, yd = owner // ny, owner % ny
    rank = (yd == y).astype(jnp.int32)
    for k in range(nz):
        rank += jnp.where(zd == far_first(nz, z, k), 2 * k, 0)
    key = rank * span + target % span
    p = jnp.arange(key.shape[0], dtype=jnp.int32)
    before = (key[None, :] < key[:, None]) | ((key[None, :] == key[:, None]) & (p[None, :] < p[:, None]))
    position = jnp.sum(before.astype(jnp.int32), axis=1)
    hit = position[None, :] == p[:, None]
    order = jnp.sum(jnp.where(hit, p[None, :], 0), axis=1)
    first = ~jnp.any((key[None, :] == key[:, None]) & (p[None, :] < p[:, None]), axis=1)
    keep = jnp.sum(jnp.where(hit & ~first[None, :], 1.0, 0.0), axis=1)
    place = jnp.arange(nz * ny * span, dtype=jnp.int32)
    upto = jnp.sum((key[None, :] <= place[:, None]).astype(jnp.int32), axis=1)
    named = jnp.any(key[None, :] == place[:, None], axis=1)
    return order, keep, jnp.where(named, upto, 0)


def fused(occ, virt, weights, occ_idx, virt_idx, target, nz, groups):
    count, terms = occ_idx.shape
    size = occ.shape[1]
    ny, span = 2, CHI_DEV
    each = UNIT
    lead = max(1, int(span // each * Z_FIRST))
    units = span // each - lead
    rows = size // groups
    block = (groups, each, rows, size)
    freqs = weights.shape[0]
    order, keep, slot = slot_tables(target, nz, span)
    smem = pl.BlockSpec(memory_space=pltpu.SMEM)
    vmem = pl.BlockSpec(memory_space=pltpu.VMEM)
    dma = pltpu.SemaphoreType.DMA
    f32 = jnp.float32
    return pl.pallas_call(
        functools.partial(fused_kernel, nz, groups, terms, 2 * count // (nz * ny)),
        out_shape=jax.ShapeDtypeStruct((freqs, span, rows, size), f32),
        in_specs=[smem] * 6 + [vmem] * 2,
        out_specs=vmem,
        scratch_shapes=[
            pltpu.VMEM((count + 1, size, size), f32),
            pltpu.VMEM((nz, units) + block, f32),
            pltpu.VMEM((nz, units) + block, f32),
            pltpu.VMEM((nz - 1, units) + block, f32),
            pltpu.VMEM((nz - 1, units) + block, f32),
            pltpu.VMEM((lead, nz, ny) + block, f32),
            pltpu.VMEM((nz - 1, ny, lead) + block, f32),
            pltpu.VMEM((nz - 1, ny, lead) + block, f32),
            pltpu.VMEM((lead,) + block, f32),
            pltpu.VMEM((units + lead,) + block, f32),
            dma((nz * units,)),
            dma((nz * units,)),
            dma((nz * units,)),
            dma(((nz - 1) * units,)),
            dma(((nz - 1) * units,)),
            dma((nz * ny * lead,)),
            dma(((nz - 1) * ny * lead,)),
            dma(((nz - 1) * ny * lead,)),
            dma((lead,)),
            dma((lead,)),
            dma(((units + lead) * groups,)),
            dma(((units + lead) * groups,)),
        ],
        compiler_params=pltpu.CompilerParams(
            collective_id=0, has_side_effects=True, vmem_limit_bytes=62 * 1024 * 1024),
    )(weights, order, keep, slot, occ_idx.T, virt_idx.T, occ, virt)


def body(occupied, virtual, cos_weights, pair_occ, pair_virt, partial_target_tile):
    owners = lax.axis_size("tile")
    groups = lax.axis_size("tau")
    size = occupied.shape[2]
    ny = 1
    while 2 * ny * 2 * ny <= owners:
        ny *= 2
    nz = owners // ny
    if ny == 2 and nz == 4:
        return fused(occupied[0], virtual[0], cos_weights, pair_occ, pair_virt,
                     partial_target_tile, nz, groups)
    tile_bytes = 4 * size * size
    span = CHI_DEV
    while span > UNIT and span * tile_bytes * (
        nz * (1 + line_slots(ny)) + line_slots(nz) + 2
    ) > BUDGET:
        span //= 2
    results = []
    for q in range(CHI_DEV // span):
        dense = products(
            occupied[0], virtual[0], pair_occ, pair_virt, partial_target_tile,
            q * span, span, min(UNIT, span), owners, groups,
        )
        results.append(scatter(dense, cos_weights, ny, nz, groups))
    return results[0] if len(results) == 1 else jnp.concatenate(results, axis=1)


def solution(mesh):
    in_specs = (
        P("tau", "tile", None, None),
        P("tau", "tile", None, None),
        P(),
        P("tile", None),
        P("tile", None),
        P("tile"),
    )
    out_specs = P(None, "tile", "tau", None)
    return jax.shard_map(body, mesh=mesh, in_specs=in_specs, out_specs=out_specs, check_vma=False)
```

```python
import functools
import math

import jax
import jax.numpy as jnp
from jax import lax
from jax.experimental import pallas as pl
from jax.experimental.pallas import tpu as pltpu
from jax.sharding import PartitionSpec as P

CHI_DEV = 32
UNIT = 2
Z_FIRST = 3 / 16
BUDGET = 46 * 1024 * 1024
MESH = pl.DeviceIdType.MESH


def products_kernel(first, terms, chi_dev, occ_idx, virt_idx, target, occ, virt, out):
    owners, units, groups, each, rows, width = out.shape
    span = units * each
    count = target.shape[0]

    @pl.loop(0, owners)
    def _(d):
        out[d] = jnp.zeros(out.shape[1:], out.dtype)

    unroll = math.gcd(count, 4) if span == chi_dev else 1

    @pl.loop(0, count, unroll=unroll)
    def _(p):
        tile = target[p]
        owner = tile // chi_dev
        place = tile - owner * chi_dev - first

        def add():
            unit = place // each
            left = [occ[occ_idx[j, p]] for j in range(terms)]
            right = [virt[virt_idx[j, p]] for j in range(terms)]
            acc = jnp.dot(
                jnp.concatenate(left, axis=1),
                jnp.concatenate(right, axis=0),
                preferred_element_type=jnp.float32,
            )
            for g in range(groups):
                out[owner, unit, g, place - unit * each] += acc[g * rows : (g + 1) * rows]

        if span == chi_dev:
            add()
        else:
            pl.when((place >= 0) & (place < span))(add)


def products(occ, virt, occ_idx, virt_idx, target, first, span, each, owners, groups):
    terms = occ_idx.shape[1]
    size = occ.shape[1]
    smem = pl.BlockSpec(memory_space=pltpu.SMEM)
    vmem = pl.BlockSpec(memory_space=pltpu.VMEM)
    return pl.pallas_call(
        functools.partial(products_kernel, first, terms, CHI_DEV),
        out_shape=jax.ShapeDtypeStruct(
            (owners, span // each, groups, each, size // groups, size), jnp.float32
        ),
        in_specs=[smem, smem, smem, vmem, vmem],
        out_specs=vmem,
        compiler_params=pltpu.CompilerParams(vmem_limit_bytes=56 * 1024 * 1024),
        cost_estimate=pl.CostEstimate(
            flops=2 * target.shape[0] * terms * size**3 * span // CHI_DEV,
            bytes_accessed=occ.size * 4 + owners * span * size * size * 4,
            transcendentals=0,
        ),
    )(occ_idx.T, virt_idx.T, target, occ, virt)


def line_slots(n):
    if n == 1:
        return 0
    return 1 if n == 2 else 2 * (n - 1)


class Line:
    def __init__(self, n, place, device, own, slots, send_sem, recv_sem, hold=None):
        self.hold = hold
        self.n, self.place, self.device = n, place, device
        self.own, self.slots, self.send_sem, self.recv_sem = own, slots, send_sem, recv_sem

    def slot(self, right, d):
        if right:
            return d - 1
        return d if self.n == 2 else self.n - 1 + d

    def copy(self, right, u, d, src, back=False):
        s = self.slot(right, d)
        k = u * line_slots(self.n) + s
        return pltpu.make_async_remote_copy(
            src_ref=src,
            dst_ref=self.slots.at[s, u],
            send_sem=self.send_sem.at[k],
            recv_sem=self.recv_sem.at[k],
            device_id={"tile": self.device(1 if right != back else -1)},
            device_id_type=MESH,
        )

    def routes(self):
        for right in (True, False):
            for d in range(self.n - 1, 0, -1) if right else range(self.n - 1):
                yield right, d

    def launch(self, u):
        for right, d in self.routes():
            @pl.when(self.place == (0 if right else self.n - 1))
            def _():
                self.copy(right, u, d, self.own(d, u)).start()

    def merge(self, u):
        if self.n == 2:
            return
        for right, d in self.routes():
            inner = (self.place > 0) & (self.place < d) if right else (
                (self.place < self.n - 1) & (self.place > d))

            @pl.when(inner)
            def _():
                here = self.slots.at[self.slot(right, d), u]
                copy = self.copy(right, u, d, here)
                copy.wait_recv()
                own = self.own(d, u)
                if self.hold is not None:
                    buffer, sem = self.hold
                    fetch = pltpu.make_async_copy(own, buffer, sem)
                    fetch.start()
                    fetch.wait()
                    own = buffer
                here[...] += own[...]
                copy.start()

    def final(self, u, into):
        for right in (True, False):
            @pl.when(self.place > 0 if right else self.place < self.n - 1)
            def _():
                k = self.slot(right, self.place)
                here = self.slots.at[k, u]
                self.copy(right, u, self.place, here, back=True).wait_recv()
                into[...] += here[...]

    def drain(self, u):
        for right, d in self.routes():
            @pl.when(self.place < d if right else self.place > d)
            def _():
                self.copy(right, u, d, self.slots.at[self.slot(right, d), u]).wait_send()


def scatter_kernel(ny, nz, groups, weights, dense, out, mine, y_slots, z_slots, times,
                   load_sem, y_send, y_recv, z_send, z_recv, t_send, t_recv, hold, hold_sem,
                   both, z2_slots, y2_slots, both_sem, z2_send, z2_recv, y2_send, y2_recv):
    tau = lax.axis_index("tau")
    tile = lax.axis_index("tile")
    z, y = tile // ny, tile % ny
    units = mine.shape[0]
    lead = both.shape[0]
    last = units - lead
    each = mine.shape[3]
    freqs = out.shape[0]

    y_line = Line(ny, y, lambda step: tile + step, lambda d, u: dense.at[:, d, u],
                  y_slots, y_send, y_recv, (hold, hold_sem))
    z_line = Line(nz, z, lambda step: tile + step * ny, lambda d, u: mine.at[u, d],
                  z_slots, z_send, z_recv)

    z2_line = Line(nz, z, z_line.device, lambda d, u: both.at[u, d], z2_slots, z2_send, z2_recv)
    y2_line = Line(ny, y, y_line.device, lambda d, u: both.at[u, z, d], y2_slots, y2_send, y2_recv)

    barrier = pltpu.get_barrier_semaphore()
    for step in range(1, groups):
        pl.semaphore_signal(barrier, inc=1, device_id={"tau": (tau + step) % groups},
                            device_id_type=MESH)
    for step in range(1, ny):
        pl.semaphore_signal(barrier, inc=1, device_id={"tile": z * ny + (y + step) % ny},
                            device_id_type=MESH)
    for step in range(1, nz):
        pl.semaphore_signal(barrier, inc=1, device_id={"tile": (z + step) % nz * ny + y},
                            device_id_type=MESH)
    pl.semaphore_wait(barrier, groups - 1 + ny - 1 + nz - 1)

    def load(u):
        return pltpu.make_async_copy(dense.at[:, y, u], mine.at[u], load_sem.at[u])

    def swap(u, step):
        other = (tau + step) % groups
        return pltpu.make_async_remote_copy(
            src_ref=mine.at[u, z, other],
            dst_ref=times.at[u, tau],
            send_sem=t_send.at[u * groups + step],
            recv_sem=t_recv.at[u * groups + tau],
            device_id={"tau": other},
            device_id_type=MESH,
        )

    def arrived(u, source):
        return pltpu.make_async_remote_copy(
            src_ref=mine.at[u, z, 0],
            dst_ref=times.at[u, source],
            send_sem=t_send.at[u * groups],
            recv_sem=t_recv.at[u * groups + source],
            device_id={"tau": source},
            device_id_type=MESH,
        )

    def whole(w):
        return pltpu.make_async_copy(dense.at[:, :, last + w], both.at[w], both_sem.at[w])

    @pl.loop(0, lead)
    def _(w):
        whole(w).start()

    @pl.loop(0, last)
    def _(u):
        y_line.launch(u)
        load(u).start()

    @pl.loop(0, lead)
    def _(w):
        whole(w).wait()
        z2_line.launch(w)

    @pl.loop(0, lead)
    def _(w):
        z2_line.merge(w)

    @pl.loop(0, units + 2)
    def _(t):
        @pl.when(t < last)
        def _():
            load(t).wait()
            y_line.merge(t)
            y_line.final(t, mine.at[t])
            z_line.launch(t)

        @pl.when(t < lead)
        def _():
            z2_line.final(t, both.at[t, z])
            y2_line.launch(t)

        @pl.when((t >= 1) & (t < last + 1))
        def _():
            u = t - 1
            z_line.merge(u)
            z_line.final(u, mine.at[u, z])

        @pl.when((t >= last + 1) & (t < units + 1))
        def _():
            w = t - 1 - last
            y2_line.merge(w)
            mine[t - 1, z] = both[w, z, y]
            y2_line.final(w, mine.at[t - 1, z])

        @pl.when((t >= 1) & (t < units + 1))
        def _():
            u = t - 1
            for step in range(1, groups):
                swap(u, step).start()
            times[u, tau] = mine[u, z, tau]

        @pl.when(t >= 2)
        def _():
            u = t - 2
            for step in range(1, groups):
                arrived(u, (tau + step) % groups).wait_recv()
            for e in range(each):
                for k in range(freqs):
                    total = weights[k, 0] * times[u, 0, e]
                    for s in range(1, groups):
                        total += weights[k, s] * times[u, s, e]
                    out[k, u * each + e] = total

    @pl.loop(0, lead)
    def _(w):
        z2_line.drain(w)
        y2_line.drain(w)

    @pl.loop(0, last)
    def _(u):
        y_line.drain(u)
        z_line.drain(u)

    @pl.loop(0, units)
    def _(u):
        for step in range(1, groups):
            swap(u, step).wait_send()


def scatter(dense, weights, ny, nz, groups):
    owners, units, _, each, rows, width = dense.shape
    freqs = weights.shape[0]
    block = (groups, each, rows, width)
    lead = max(1, int(units * Z_FIRST))
    ys, zs = max(line_slots(ny), 1), max(line_slots(nz), 1)
    dma = pltpu.SemaphoreType.DMA
    return pl.pallas_call(
        functools.partial(scatter_kernel, ny, nz, groups),
        out_shape=jax.ShapeDtypeStruct((freqs, units * each, rows, width), jnp.float32),
        in_specs=[pl.BlockSpec(memory_space=pltpu.SMEM), pl.BlockSpec(memory_space=pl.ANY)],
        out_specs=pl.BlockSpec(memory_space=pltpu.VMEM),
        scratch_shapes=[
            pltpu.VMEM((units, nz) + block, jnp.float32),
            pltpu.VMEM((ys, units, nz) + block, jnp.float32),
            pltpu.VMEM((zs, units) + block, jnp.float32),
            pltpu.VMEM((units, groups, each, rows, width), jnp.float32),
            dma((units,)),
            dma((units * ys,)),
            dma((units * ys,)),
            dma((units * zs,)),
            dma((units * zs,)),
            dma((units * groups,)),
            dma((units * groups,)),
            pltpu.VMEM((nz,) + block if ny > 2 else (8, 128), jnp.float32),
            dma,
            pltpu.VMEM((lead, nz, ny) + block, jnp.float32),
            pltpu.VMEM((zs, lead, ny) + block, jnp.float32),
            pltpu.VMEM((ys, lead) + block, jnp.float32),
            dma((lead,)),
            dma((lead * zs,)),
            dma((lead * zs,)),
            dma((lead * ys,)),
            dma((lead * ys,)),
        ],
        compiler_params=pltpu.CompilerParams(
            collective_id=0, has_side_effects=True, vmem_limit_bytes=58 * 1024 * 1024),
    )(weights, dense.reshape((nz, ny) + dense.shape[1:]))


def far_first(nz, z, k):
    flip = z // (nz // 2)
    m = z + flip * (nz - 1 - 2 * z)
    ends = nz - 1 - k
    inner = (1 - k % 2) * (nz - 1 - k // 2) + (k % 2) * (k // 2)
    e = (1 - m) * ends + m * inner
    return e + flip * (nz - 1 - 2 * e)


def fused_kernel(nz, groups, terms, cap, weights, order, slot, occ_idx, virt_idx, occ_hbm, virt_hbm,
                 out, occ, virt, load_sem, packed, y_out, y_in, z_right, z_left, lead_own, z2_right, z2_left, y2_in,
                 times, y_send, y_recv, z_send, zr_recv, zl_recv, z2_send, z2r_recv, z2l_recv,
                 y2_send, y2_recv, t_send, t_recv):
    tau = lax.axis_index("tau")
    tile = lax.axis_index("tile")
    ny = 2
    z, y = tile // ny, tile % ny
    other_y = 1 - y
    lead = lead_own.shape[0]
    units = y_out.shape[1]
    each, rows = y_out.shape[3], y_out.shape[4]
    span = (units + lead) * each
    owners = nz * ny
    count = order.shape[0]
    freqs = out.shape[0]

    def dest(k):
        return far_first(nz, z, k)

    def remote(src, dst, send, recv, device):
        return pltpu.make_async_remote_copy(
            src_ref=src, dst_ref=dst, send_sem=send, recv_sem=recv,
            device_id=device, device_id_type=MESH)

    def y_copy(d, u):
        k = d * units + u
        return remote(y_out.at[d, u], y_in.at[d, u], y_send.at[k], y_recv.at[k],
                      {"tile": z * ny + other_y})

    def z_copy(right, d, u, src, back=False):
        if right:
            k = (d - 1) * units + u
            dst, recv = z_right.at[d - 1, u], zr_recv.at[k]
        else:
            k = d * units + u
            dst, recv = z_left.at[d, u], zl_recv.at[k]
        return remote(src, dst, z_send.at[d * units + u], recv,
                      {"tile": tile + (ny if right != back else -ny)})

    def z2_copy(right, d, yy, w, src, back=False):
        k = (d * ny + yy) * lead + w
        if right:
            dst, recv = z2_right.at[d - 1, yy, w], z2r_recv.at[k - ny * lead]
        else:
            dst, recv = z2_left.at[d, yy, w], z2l_recv.at[k]
        return remote(src, dst, z2_send.at[k], recv,
                      {"tile": tile + (ny if right != back else -ny)})

    def y2_copy(w):
        return remote(lead_own.at[w, z, other_y], y2_in.at[w], y2_send.at[w], y2_recv.at[w],
                      {"tile": z * ny + other_y})

    def swap(src, u, step):
        other = (tau + step) % groups
        return remote(src.at[other], times.at[u, tau], t_send.at[u * groups + step],
                      t_recv.at[u * groups + tau], {"tau": other})

    def arrived(u, source):
        return remote(times.at[u, tau], times.at[u, source], t_send.at[u * groups],
                      t_recv.at[u * groups + source], {"tau": source})

    loads = [pltpu.make_async_copy(occ_hbm, occ, load_sem.at[0]),
             pltpu.make_async_copy(virt_hbm, virt, load_sem.at[1])]
    for load in loads:
        load.start()

    barrier = pltpu.get_barrier_semaphore()
    for step in range(1, groups):
        pl.semaphore_signal(barrier, inc=1, device_id={"tau": (tau + step) % groups},
                            device_id_type=MESH)
    pl.semaphore_signal(barrier, inc=1, device_id={"tile": z * ny + other_y}, device_id_type=MESH)
    for step in range(1, nz):
        pl.semaphore_signal(barrier, inc=1, device_id={"tile": (z + step) % nz * ny + y},
                            device_id_type=MESH)
    pl.semaphore_wait(barrier, groups - 1 + ny - 1 + nz - 1)

    packed[0] = jnp.zeros(packed.shape[1:], packed.dtype)
    for load in loads:
        load.wait()

    def product(s):
        p = order[s] // 2
        keep = (order[s] % 2).astype(jnp.float32)
        left = [occ[occ_idx[j, p]] for j in range(terms)]
        right = [virt[virt_idx[j, p]] for j in range(terms)]
        acc = jnp.dot(
            jnp.concatenate(left, axis=1),
            jnp.concatenate(right, axis=0),
            preferred_element_type=jnp.float32,
        )
        packed[s + 1] = acc + keep * packed[s]

    def fill(rank, u, ref, add):
        for e in range(each):
            part = packed[slot[rank * span + u * each + e]]
            for g in range(groups):
                piece = part[g * rows:(g + 1) * rows]
                if add:
                    ref[g, e] += piece
                else:
                    ref[g, e] = piece

    def ready(rank):
        d = dest(rank // 2)
        yy = y if rank % 2 else other_y
        if rank % 2 == 0:
            @pl.loop(0, units)
            def _(u):
                fill(rank, u, y_out.at[d, u], False)
                if rank < owners - ny:
                    y_copy(d, u).start()

        @pl.loop(0, lead)
        def _(w):
            own = lead_own.at[w, d, yy]
            fill(rank, units + w, own, False)

            @pl.when((z == 0) & (d > z))
            def _():
                z2_copy(True, d, yy, w, own).start()

            @pl.when((z == nz - 1) & (d < z))
            def _():
                z2_copy(False, d, yy, w, own).start()

    def y_stage(i):
        k, u = i // units, i % units
        d = dest(k)
        here = y_in.at[d, u]
        y_copy(d, u).wait_recv()
        fill(2 * k + 1, u, here, True)

        @pl.when((z == 0) & (d > z))
        def _():
            z_copy(True, d, u, here).start()

        @pl.when((z == nz - 1) & (d < z))
        def _():
            z_copy(False, d, u, here).start()

    def z_stage(i):
        k, u = i // units, i % units
        d = dest(k)
        own = y_in.at[d, u]

        @pl.when((z > 0) & (d > z))
        def _():
            here = z_right.at[d - 1, u]
            copy = z_copy(True, d, u, here)
            copy.wait_recv()
            here[...] += own[...]
            copy.start()

        @pl.when((z < nz - 1) & (d < z))
        def _():
            here = z_left.at[d, u]
            copy = z_copy(False, d, u, here)
            copy.wait_recv()
            here[...] += own[...]
            copy.start()

        @pl.when((d == z) & (z > 0))
        def _():
            here = z_right.at[z - 1, u]
            z_copy(True, z, u, here, True).wait_recv()
            own[...] += here[...]

        @pl.when((d == z) & (z < nz - 1))
        def _():
            here = z_left.at[z, u]
            z_copy(False, z, u, here, True).wait_recv()
            own[...] += here[...]

        @pl.when(d == z)
        def _():
            for step in range(1, groups):
                swap(own, u, step).start()
            times[u, tau] = own[tau]

    def lead_stage(j):
        rank, w = j // lead, j % lead
        d = dest(rank // 2)
        yy = y + (1 - rank % 2) * (1 - 2 * y)
        own = lead_own.at[w, d, yy]

        @pl.when((z > 0) & (d > z))
        def _():
            here = z2_right.at[d - 1, yy, w]
            copy = z2_copy(True, d, yy, w, here)
            copy.wait_recv()
            here[...] += own[...]
            copy.start()

        @pl.when((z < nz - 1) & (d < z))
        def _():
            here = z2_left.at[d, yy, w]
            copy = z2_copy(False, d, yy, w, here)
            copy.wait_recv()
            here[...] += own[...]
            copy.start()

        @pl.when((d == z) & (z > 0))
        def _():
            here = z2_right.at[z - 1, yy, w]
            z2_copy(True, z, yy, w, here, True).wait_recv()
            own[...] += here[...]

        @pl.when((d == z) & (z < nz - 1))
        def _():
            here = z2_left.at[z, yy, w]
            z2_copy(False, z, yy, w, here, True).wait_recv()
            own[...] += here[...]

        @pl.when((d == z) & (rank % 2 == 0))
        def _():
            y2_copy(w).start()

    def cross_stage(w):
        own = lead_own.at[w, z, y]
        y2_copy(w).wait_recv()
        own[...] += y2_in[w]
        for step in range(1, groups):
            swap(own, units + w, step).start()
        times[units + w, tau] = own[tau]

    def out_stage(u):
        for step in range(1, groups):
            arrived(u, (tau + step) % groups).wait_recv()
        for e in range(each):
            for k in range(freqs):
                total = weights[k, 0] * times[u, 0, e]
                for s in range(1, groups):
                    total += weights[k, s] * times[u, s, e]
                out[k, u * each + e] = total

    early = 0
    phases = -(-count // cap)
    for phase in range(phases):
        @pl.loop(phase * cap, min(count, (phase + 1) * cap), unroll=8)
        def _(s):
            product(s)

        for rank in range(phase, phase + 1 if phase < phases - 1 else owners):
            ready(rank)
        upto = early
        if 1 <= phase < phases - 1:
            upto = early + 2 * phase

            @pl.loop(early, upto)
            def _(i):
                y_stage(i)
        early = upto

    items = nz * units
    passing = items - units
    hold, lag = 2, 3
    last = early + owners * lead

    @pl.loop(early, items + lag + hold)
    def _(t):
        @pl.when(t < items)
        def _():
            y_stage(t)

        @pl.when(t < last)
        def _():
            lead_stage(t - early)

        @pl.when(t == last)
        def _():
            @pl.loop(0, units)
            def _(u):
                y_copy(z, u).start()

        @pl.when(t < passing + early)
        def _():
            z_stage(t - early)

        @pl.when((t >= passing + lag) & (t < items + lag))
        def _():
            z_stage(t - lag)

        @pl.when((t >= passing + early) & (t < passing + early + lead))
        def _():
            cross_stage(t - passing - early)

        @pl.when((t >= passing + early + hold) & (t < passing + early + hold + lead))
        def _():
            out_stage(t - passing - early - hold + units)

        @pl.when(t >= passing + lag + hold)
        def _():
            out_stage(t - passing - lag - hold)

    @pl.loop(0, units)
    def _(u):
        @pl.loop(0, nz)
        def _(d):
            y_copy(d, u).wait_send()

            @pl.when(d > z)
            def _():
                z_copy(True, d, u, y_in.at[d, u]).wait_send()

            @pl.when(d < z)
            def _():
                z_copy(False, d, u, y_in.at[d, u]).wait_send()

        for step in range(1, groups):
            swap(y_in.at[z, u], u, step).wait_send()

    @pl.loop(0, lead)
    def _(w):
        @pl.loop(0, nz)
        def _(d):
            for yy in range(ny):
                @pl.when(d > z)
                def _():
                    z2_copy(True, d, yy, w, lead_own.at[w, d, yy]).wait_send()

                @pl.when(d < z)
                def _():
                    z2_copy(False, d, yy, w, lead_own.at[w, d, yy]).wait_send()

        y2_copy(w).wait_send()
        for step in range(1, groups):
            swap(lead_own.at[w, z, y], units + w, step).wait_send()


def slot_tables(target, nz, span):
    ny = 2
    tile = lax.axis_index("tile")
    z, y = tile // ny, tile % ny
    owner = target // span
    zd, yd = owner // ny, owner % ny
    rank = (yd == y).astype(jnp.int32)
    for k in range(nz):
        rank += jnp.where(zd == far_first(nz, z, k), 2 * k, 0)
    key = rank * span + target % span
    p = jnp.arange(key.shape[0], dtype=jnp.int32)
    before = (key[None, :] < key[:, None]) | ((key[None, :] == key[:, None]) & (p[None, :] < p[:, None]))
    position = jnp.sum(before.astype(jnp.int32), axis=1)
    again = jnp.any((key[None, :] == key[:, None]) & (p[None, :] < p[:, None]), axis=1)
    code = 2 * p + again.astype(jnp.int32)
    order = jnp.sum(jnp.where(position[None, :] == p[:, None], code[None, :], 0), axis=1)
    place = jnp.arange(nz * ny * span, dtype=jnp.int32)
    big = 2 * key.shape[0]
    found = jnp.sum((key[None, :] <= place[:, None]).astype(jnp.int32)
                    + jnp.where(key[None, :] == place[:, None], big, 0), axis=1)
    return order, jnp.where(found >= big, found % big, 0)


def fused(occ, virt, weights, occ_idx, virt_idx, target, nz, groups):
    count, terms = occ_idx.shape
    size = occ.shape[1]
    ny, span = 2, CHI_DEV
    each = UNIT
    lead = max(1, int(span // each * Z_FIRST))
    units = span // each - lead
    rows = size // groups
    block = (groups, each, rows, size)
    freqs = weights.shape[0]
    order, slot = slot_tables(target, nz, span)
    smem = pl.BlockSpec(memory_space=pltpu.SMEM)
    vmem = pl.BlockSpec(memory_space=pltpu.VMEM)
    dma = pltpu.SemaphoreType.DMA
    f32 = jnp.float32
    return pl.pallas_call(
        functools.partial(fused_kernel, nz, groups, terms, 2 * count // (nz * ny)),
        out_shape=jax.ShapeDtypeStruct((freqs, span, rows, size), f32),
        in_specs=[smem] * 5 + [pl.BlockSpec(memory_space=pl.ANY)] * 2,
        out_specs=vmem,
        scratch_shapes=[
            pltpu.VMEM(occ.shape, occ.dtype),
            pltpu.VMEM(virt.shape, virt.dtype),
            dma((2,)),
            pltpu.VMEM((count + 1, size, size), f32),
            pltpu.VMEM((nz, units) + block, f32),
            pltpu.VMEM((nz, units) + block, f32),
            pltpu.VMEM((nz - 1, units) + block, f32),
            pltpu.VMEM((nz - 1, units) + block, f32),
            pltpu.VMEM((lead, nz, ny) + block, f32),
            pltpu.VMEM((nz - 1, ny, lead) + block, f32),
            pltpu.VMEM((nz - 1, ny, lead) + block, f32),
            pltpu.VMEM((lead,) + block, f32),
            pltpu.VMEM((units + lead,) + block, f32),
            dma((nz * units,)),
            dma((nz * units,)),
            dma((nz * units,)),
            dma(((nz - 1) * units,)),
            dma(((nz - 1) * units,)),
            dma((nz * ny * lead,)),
            dma(((nz - 1) * ny * lead,)),
            dma(((nz - 1) * ny * lead,)),
            dma((lead,)),
            dma((lead,)),
            dma(((units + lead) * groups,)),
            dma(((units + lead) * groups,)),
        ],
        compiler_params=pltpu.CompilerParams(
            collective_id=0, has_side_effects=True, vmem_limit_bytes=62 * 1024 * 1024),
    )(weights, order, slot, occ_idx.T, virt_idx.T, occ, virt)


def body(occupied, virtual, cos_weights, pair_occ, pair_virt, partial_target_tile):
    owners = lax.axis_size("tile")
    groups = lax.axis_size("tau")
    size = occupied.shape[2]
    ny = 1
    while 2 * ny * 2 * ny <= owners:
        ny *= 2
    nz = owners // ny
    if ny == 2 and nz == 4:
        return fused(occupied[0], virtual[0], cos_weights, pair_occ, pair_virt,
                     partial_target_tile, nz, groups)
    tile_bytes = 4 * size * size
    span = CHI_DEV
    while span > UNIT and span * tile_bytes * (
        nz * (1 + line_slots(ny)) + line_slots(nz) + 2
    ) > BUDGET:
        span //= 2
    results = []
    for q in range(CHI_DEV // span):
        dense = products(
            occupied[0], virtual[0], pair_occ, pair_virt, partial_target_tile,
            q * span, span, min(UNIT, span), owners, groups,
        )
        results.append(scatter(dense, cos_weights, ny, nz, groups))
    return results[0] if len(results) == 1 else jnp.concatenate(results, axis=1)


def solution(mesh):
    in_specs = (
        P("tau", "tile", None, None),
        P("tau", "tile", None, None),
        P(),
        P("tile", None),
        P("tile", None),
        P("tile"),
    )
    out_specs = P(None, "tile", "tau", None)
    return jax.shard_map(body, mesh=mesh, in_specs=in_specs, out_specs=out_specs, check_vma=False)
```

```python
import functools
import math

import jax
import jax.numpy as jnp
from jax import lax
from jax.experimental import pallas as pl
from jax.experimental.pallas import tpu as pltpu
from jax.sharding import PartitionSpec as P

CHI_DEV = 32
UNIT = 2
Z_FIRST = 3 / 16
BUDGET = 46 * 1024 * 1024
MESH = pl.DeviceIdType.MESH


def products_kernel(first, terms, chi_dev, occ_idx, virt_idx, target, occ, virt, out):
    owners, units, groups, each, rows, width = out.shape
    span = units * each
    count = target.shape[0]

    @pl.loop(0, owners)
    def _(d):
        out[d] = jnp.zeros(out.shape[1:], out.dtype)

    unroll = math.gcd(count, 4) if span == chi_dev else 1

    @pl.loop(0, count, unroll=unroll)
    def _(p):
        tile = target[p]
        owner = tile // chi_dev
        place = tile - owner * chi_dev - first

        def add():
            unit = place // each
            left = [occ[occ_idx[j, p]] for j in range(terms)]
            right = [virt[virt_idx[j, p]] for j in range(terms)]
            acc = jnp.dot(
                jnp.concatenate(left, axis=1),
                jnp.concatenate(right, axis=0),
                preferred_element_type=jnp.float32,
            )
            for g in range(groups):
                out[owner, unit, g, place - unit * each] += acc[g * rows : (g + 1) * rows]

        if span == chi_dev:
            add()
        else:
            pl.when((place >= 0) & (place < span))(add)


def products(occ, virt, occ_idx, virt_idx, target, first, span, each, owners, groups):
    terms = occ_idx.shape[1]
    size = occ.shape[1]
    smem = pl.BlockSpec(memory_space=pltpu.SMEM)
    vmem = pl.BlockSpec(memory_space=pltpu.VMEM)
    return pl.pallas_call(
        functools.partial(products_kernel, first, terms, CHI_DEV),
        out_shape=jax.ShapeDtypeStruct(
            (owners, span // each, groups, each, size // groups, size), jnp.float32
        ),
        in_specs=[smem, smem, smem, vmem, vmem],
        out_specs=vmem,
        compiler_params=pltpu.CompilerParams(vmem_limit_bytes=56 * 1024 * 1024),
        cost_estimate=pl.CostEstimate(
            flops=2 * target.shape[0] * terms * size**3 * span // CHI_DEV,
            bytes_accessed=occ.size * 4 + owners * span * size * size * 4,
            transcendentals=0,
        ),
    )(occ_idx.T, virt_idx.T, target, occ, virt)


def line_slots(n):
    if n == 1:
        return 0
    return 1 if n == 2 else 2 * (n - 1)


class Line:
    def __init__(self, n, place, device, own, slots, send_sem, recv_sem, hold=None):
        self.hold = hold
        self.n, self.place, self.device = n, place, device
        self.own, self.slots, self.send_sem, self.recv_sem = own, slots, send_sem, recv_sem

    def slot(self, right, d):
        if right:
            return d - 1
        return d if self.n == 2 else self.n - 1 + d

    def copy(self, right, u, d, src, back=False):
        s = self.slot(right, d)
        k = u * line_slots(self.n) + s
        return pltpu.make_async_remote_copy(
            src_ref=src,
            dst_ref=self.slots.at[s, u],
            send_sem=self.send_sem.at[k],
            recv_sem=self.recv_sem.at[k],
            device_id={"tile": self.device(1 if right != back else -1)},
            device_id_type=MESH,
        )

    def routes(self):
        for right in (True, False):
            for d in range(self.n - 1, 0, -1) if right else range(self.n - 1):
                yield right, d

    def launch(self, u):
        for right, d in self.routes():
            @pl.when(self.place == (0 if right else self.n - 1))
            def _():
                self.copy(right, u, d, self.own(d, u)).start()

    def merge(self, u):
        if self.n == 2:
            return
        for right, d in self.routes():
            inner = (self.place > 0) & (self.place < d) if right else (
                (self.place < self.n - 1) & (self.place > d))

            @pl.when(inner)
            def _():
                here = self.slots.at[self.slot(right, d), u]
                copy = self.copy(right, u, d, here)
                copy.wait_recv()
                own = self.own(d, u)
                if self.hold is not None:
                    buffer, sem = self.hold
                    fetch = pltpu.make_async_copy(own, buffer, sem)
                    fetch.start()
                    fetch.wait()
                    own = buffer
                here[...] += own[...]
                copy.start()

    def final(self, u, into):
        for right in (True, False):
            @pl.when(self.place > 0 if right else self.place < self.n - 1)
            def _():
                k = self.slot(right, self.place)
                here = self.slots.at[k, u]
                self.copy(right, u, self.place, here, back=True).wait_recv()
                into[...] += here[...]

    def drain(self, u):
        for right, d in self.routes():
            @pl.when(self.place < d if right else self.place > d)
            def _():
                self.copy(right, u, d, self.slots.at[self.slot(right, d), u]).wait_send()


def scatter_kernel(ny, nz, groups, weights, dense, out, mine, y_slots, z_slots, times,
                   load_sem, y_send, y_recv, z_send, z_recv, t_send, t_recv, hold, hold_sem,
                   both, z2_slots, y2_slots, both_sem, z2_send, z2_recv, y2_send, y2_recv):
    tau = lax.axis_index("tau")
    tile = lax.axis_index("tile")
    z, y = tile // ny, tile % ny
    units = mine.shape[0]
    lead = both.shape[0]
    last = units - lead
    each = mine.shape[3]
    freqs = out.shape[0]

    y_line = Line(ny, y, lambda step: tile + step, lambda d, u: dense.at[:, d, u],
                  y_slots, y_send, y_recv, (hold, hold_sem))
    z_line = Line(nz, z, lambda step: tile + step * ny, lambda d, u: mine.at[u, d],
                  z_slots, z_send, z_recv)

    z2_line = Line(nz, z, z_line.device, lambda d, u: both.at[u, d], z2_slots, z2_send, z2_recv)
    y2_line = Line(ny, y, y_line.device, lambda d, u: both.at[u, z, d], y2_slots, y2_send, y2_recv)

    barrier = pltpu.get_barrier_semaphore()
    for step in range(1, groups):
        pl.semaphore_signal(barrier, inc=1, device_id={"tau": (tau + step) % groups},
                            device_id_type=MESH)
    for step in range(1, ny):
        pl.semaphore_signal(barrier, inc=1, device_id={"tile": z * ny + (y + step) % ny},
                            device_id_type=MESH)
    for step in range(1, nz):
        pl.semaphore_signal(barrier, inc=1, device_id={"tile": (z + step) % nz * ny + y},
                            device_id_type=MESH)
    pl.semaphore_wait(barrier, groups - 1 + ny - 1 + nz - 1)

    def load(u):
        return pltpu.make_async_copy(dense.at[:, y, u], mine.at[u], load_sem.at[u])

    def swap(u, step):
        other = (tau + step) % groups
        return pltpu.make_async_remote_copy(
            src_ref=mine.at[u, z, other],
            dst_ref=times.at[u, tau],
            send_sem=t_send.at[u * groups + step],
            recv_sem=t_recv.at[u * groups + tau],
            device_id={"tau": other},
            device_id_type=MESH,
        )

    def arrived(u, source):
        return pltpu.make_async_remote_copy(
            src_ref=mine.at[u, z, 0],
            dst_ref=times.at[u, source],
            send_sem=t_send.at[u * groups],
            recv_sem=t_recv.at[u * groups + source],
            device_id={"tau": source},
            device_id_type=MESH,
        )

    def whole(w):
        return pltpu.make_async_copy(dense.at[:, :, last + w], both.at[w], both_sem.at[w])

    @pl.loop(0, lead)
    def _(w):
        whole(w).start()

    @pl.loop(0, last)
    def _(u):
        y_line.launch(u)
        load(u).start()

    @pl.loop(0, lead)
    def _(w):
        whole(w).wait()
        z2_line.launch(w)

    @pl.loop(0, lead)
    def _(w):
        z2_line.merge(w)

    @pl.loop(0, units + 2)
    def _(t):
        @pl.when(t < last)
        def _():
            load(t).wait()
            y_line.merge(t)
            y_line.final(t, mine.at[t])
            z_line.launch(t)

        @pl.when(t < lead)
        def _():
            z2_line.final(t, both.at[t, z])
            y2_line.launch(t)

        @pl.when((t >= 1) & (t < last + 1))
        def _():
            u = t - 1
            z_line.merge(u)
            z_line.final(u, mine.at[u, z])

        @pl.when((t >= last + 1) & (t < units + 1))
        def _():
            w = t - 1 - last
            y2_line.merge(w)
            mine[t - 1, z] = both[w, z, y]
            y2_line.final(w, mine.at[t - 1, z])

        @pl.when((t >= 1) & (t < units + 1))
        def _():
            u = t - 1
            for step in range(1, groups):
                swap(u, step).start()
            times[u, tau] = mine[u, z, tau]

        @pl.when(t >= 2)
        def _():
            u = t - 2
            for step in range(1, groups):
                arrived(u, (tau + step) % groups).wait_recv()
            for e in range(each):
                for k in range(freqs):
                    total = weights[k, 0] * times[u, 0, e]
                    for s in range(1, groups):
                        total += weights[k, s] * times[u, s, e]
                    out[k, u * each + e] = total

    @pl.loop(0, lead)
    def _(w):
        z2_line.drain(w)
        y2_line.drain(w)

    @pl.loop(0, last)
    def _(u):
        y_line.drain(u)
        z_line.drain(u)

    @pl.loop(0, units)
    def _(u):
        for step in range(1, groups):
            swap(u, step).wait_send()


def scatter(dense, weights, ny, nz, groups):
    owners, units, _, each, rows, width = dense.shape
    freqs = weights.shape[0]
    block = (groups, each, rows, width)
    lead = max(1, int(units * Z_FIRST))
    ys, zs = max(line_slots(ny), 1), max(line_slots(nz), 1)
    dma = pltpu.SemaphoreType.DMA
    return pl.pallas_call(
        functools.partial(scatter_kernel, ny, nz, groups),
        out_shape=jax.ShapeDtypeStruct((freqs, units * each, rows, width), jnp.float32),
        in_specs=[pl.BlockSpec(memory_space=pltpu.SMEM), pl.BlockSpec(memory_space=pl.ANY)],
        out_specs=pl.BlockSpec(memory_space=pltpu.VMEM),
        scratch_shapes=[
            pltpu.VMEM((units, nz) + block, jnp.float32),
            pltpu.VMEM((ys, units, nz) + block, jnp.float32),
            pltpu.VMEM((zs, units) + block, jnp.float32),
            pltpu.VMEM((units, groups, each, rows, width), jnp.float32),
            dma((units,)),
            dma((units * ys,)),
            dma((units * ys,)),
            dma((units * zs,)),
            dma((units * zs,)),
            dma((units * groups,)),
            dma((units * groups,)),
            pltpu.VMEM((nz,) + block if ny > 2 else (8, 128), jnp.float32),
            dma,
            pltpu.VMEM((lead, nz, ny) + block, jnp.float32),
            pltpu.VMEM((zs, lead, ny) + block, jnp.float32),
            pltpu.VMEM((ys, lead) + block, jnp.float32),
            dma((lead,)),
            dma((lead * zs,)),
            dma((lead * zs,)),
            dma((lead * ys,)),
            dma((lead * ys,)),
        ],
        compiler_params=pltpu.CompilerParams(
            collective_id=0, has_side_effects=True, vmem_limit_bytes=58 * 1024 * 1024),
    )(weights, dense.reshape((nz, ny) + dense.shape[1:]))


def far_first(nz, z, k):
    flip = z // (nz // 2)
    m = z + flip * (nz - 1 - 2 * z)
    ends = nz - 1 - k
    inner = (1 - k % 2) * (nz - 1 - k // 2) + (k % 2) * (k // 2)
    e = (1 - m) * ends + m * inner
    return e + flip * (nz - 1 - 2 * e)


def fused_kernel(nz, groups, terms, cap, weights, order, slot, occ_idx, virt_idx, occ_hbm, virt_hbm,
                 out, occ, virt, load_sem, packed, y_out, y_in, z_right, z_left, lead_own, z2_right, z2_left, y2_in,
                 times, y_send, y_recv, z_send, zr_recv, zl_recv, z2_send, z2r_recv, z2l_recv,
                 y2_send, y2_recv, t_send, t_recv):
    tau = lax.axis_index("tau")
    tile = lax.axis_index("tile")
    ny = 2
    z, y = tile // ny, tile % ny
    other_y = 1 - y
    lead = lead_own.shape[0]
    units = y_out.shape[1]
    each, rows = y_out.shape[3], y_out.shape[4]
    span = (units + lead) * each
    owners = nz * ny
    count = order.shape[0]
    freqs = out.shape[0]

    def dest(k):
        return far_first(nz, z, k)

    def remote(src, dst, send, recv, device):
        return pltpu.make_async_remote_copy(
            src_ref=src, dst_ref=dst, send_sem=send, recv_sem=recv,
            device_id=device, device_id_type=MESH)

    def y_copy(d, u):
        k = d * units + u
        return remote(y_out.at[d, u], y_in.at[d, u], y_send.at[k], y_recv.at[k],
                      {"tile": z * ny + other_y})

    def z_copy(right, d, u, src, back=False):
        if right:
            k = (d - 1) * units + u
            dst, recv = z_right.at[d - 1, u], zr_recv.at[k]
        else:
            k = d * units + u
            dst, recv = z_left.at[d, u], zl_recv.at[k]
        return remote(src, dst, z_send.at[d * units + u], recv,
                      {"tile": tile + (ny if right != back else -ny)})

    def z2_copy(right, d, yy, w, src, back=False):
        k = (d * ny + yy) * lead + w
        if right:
            dst, recv = z2_right.at[d - 1, yy, w], z2r_recv.at[k - ny * lead]
        else:
            dst, recv = z2_left.at[d, yy, w], z2l_recv.at[k]
        return remote(src, dst, z2_send.at[k], recv,
                      {"tile": tile + (ny if right != back else -ny)})

    def y2_copy(w):
        return remote(lead_own.at[w, z, other_y], y2_in.at[w], y2_send.at[w], y2_recv.at[w],
                      {"tile": z * ny + other_y})

    def swap(src, u, step):
        other = (tau + step) % groups
        return remote(src.at[other], times.at[u, tau], t_send.at[u * groups + step],
                      t_recv.at[u * groups + tau], {"tau": other})

    def arrived(u, source):
        return remote(times.at[u, tau], times.at[u, source], t_send.at[u * groups],
                      t_recv.at[u * groups + source], {"tau": source})

    loads = [pltpu.make_async_copy(occ_hbm, occ, load_sem.at[0]),
             pltpu.make_async_copy(virt_hbm, virt, load_sem.at[1])]
    for load in loads:
        load.start()

    barrier = pltpu.get_barrier_semaphore()
    for step in range(1, groups):
        pl.semaphore_signal(barrier, inc=1, device_id={"tau": (tau + step) % groups},
                            device_id_type=MESH)
    pl.semaphore_signal(barrier, inc=1, device_id={"tile": z * ny + other_y}, device_id_type=MESH)
    @pl.when(z > 0)
    def _():
        pl.semaphore_signal(barrier, inc=1, device_id={"tile": tile - ny}, device_id_type=MESH)

    @pl.when(z < nz - 1)
    def _():
        pl.semaphore_signal(barrier, inc=1, device_id={"tile": tile + ny}, device_id_type=MESH)

    beside = (z + nz - 1) // nz + (2 * nz - 2 - z) // nz
    pl.semaphore_wait(barrier, groups - 1 + ny - 1 + beside)

    packed[0] = jnp.zeros(packed.shape[1:], packed.dtype)
    for load in loads:
        load.wait()

    def product(s):
        p = order[s] // 2
        keep = (order[s] % 2).astype(jnp.float32)
        left = [occ[occ_idx[j, p]] for j in range(terms)]
        right = [virt[virt_idx[j, p]] for j in range(terms)]
        acc = jnp.dot(
            jnp.concatenate(left, axis=1),
            jnp.concatenate(right, axis=0),
            preferred_element_type=jnp.float32,
        )
        packed[s + 1] = acc + keep * packed[s]

    def fill(rank, u, ref, add):
        for e in range(each):
            part = packed[slot[rank * span + u * each + e]]
            for g in range(groups):
                piece = part[g * rows:(g + 1) * rows]
                if add:
                    ref[g, e] += piece
                else:
                    ref[g, e] = piece

    def ready(rank):
        d = dest(rank // 2)
        yy = y if rank % 2 else other_y
        if rank % 2 == 0:
            @pl.loop(0, units)
            def _(u):
                fill(rank, u, y_out.at[d, u], False)
                if rank < owners - ny:
                    y_copy(d, u).start()

        @pl.loop(0, lead)
        def _(w):
            own = lead_own.at[w, d, yy]
            fill(rank, units + w, own, False)

            @pl.when((z == 0) & (d > z))
            def _():
                z2_copy(True, d, yy, w, own).start()

            @pl.when((z == nz - 1) & (d < z))
            def _():
                z2_copy(False, d, yy, w, own).start()

    def y_stage(i):
        k, u = i // units, i % units
        d = dest(k)
        here = y_in.at[d, u]
        y_copy(d, u).wait_recv()
        fill(2 * k + 1, u, here, True)

        @pl.when((z == 0) & (d > z))
        def _():
            z_copy(True, d, u, here).start()

        @pl.when((z == nz - 1) & (d < z))
        def _():
            z_copy(False, d, u, here).start()

    def z_stage(i):
        k, u = i // units, i % units
        d = dest(k)
        own = y_in.at[d, u]

        @pl.when((z > 0) & (d > z))
        def _():
            here = z_right.at[d - 1, u]
            copy = z_copy(True, d, u, here)
            copy.wait_recv()
            here[...] += own[...]
            copy.start()

        @pl.when((z < nz - 1) & (d < z))
        def _():
            here = z_left.at[d, u]
            copy = z_copy(False, d, u, here)
            copy.wait_recv()
            here[...] += own[...]
            copy.start()

        @pl.when((d == z) & (z > 0))
        def _():
            here = z_right.at[z - 1, u]
            z_copy(True, z, u, here, True).wait_recv()
            own[...] += here[...]

        @pl.when((d == z) & (z < nz - 1))
        def _():
            here = z_left.at[z, u]
            z_copy(False, z, u, here, True).wait_recv()
            own[...] += here[...]

        @pl.when(d == z)
        def _():
            for step in range(1, groups):
                swap(own, u, step).start()
            times[u, tau] = own[tau]

    def lead_stage(j):
        rank, w = j // lead, j % lead
        d = dest(rank // 2)
        yy = y + (1 - rank % 2) * (1 - 2 * y)
        own = lead_own.at[w, d, yy]

        @pl.when((z > 0) & (d > z))
        def _():
            here = z2_right.at[d - 1, yy, w]
            copy = z2_copy(True, d, yy, w, here)
            copy.wait_recv()
            here[...] += own[...]
            copy.start()

        @pl.when((z < nz - 1) & (d < z))
        def _():
            here = z2_left.at[d, yy, w]
            copy = z2_copy(False, d, yy, w, here)
            copy.wait_recv()
            here[...] += own[...]
            copy.start()

        @pl.when((d == z) & (z > 0))
        def _():
            here = z2_right.at[z - 1, yy, w]
            z2_copy(True, z, yy, w, here, True).wait_recv()
            own[...] += here[...]

        @pl.when((d == z) & (z < nz - 1))
        def _():
            here = z2_left.at[z, yy, w]
            z2_copy(False, z, yy, w, here, True).wait_recv()
            own[...] += here[...]

        @pl.when((d == z) & (rank % 2 == 0))
        def _():
            y2_copy(w).start()

    def cross_stage(w):
        own = lead_own.at[w, z, y]
        y2_copy(w).wait_recv()
        own[...] += y2_in[w]
        for step in range(1, groups):
            swap(own, units + w, step).start()
        times[units + w, tau] = own[tau]

    def out_stage(u):
        for step in range(1, groups):
            arrived(u, (tau + step) % groups).wait_recv()
        for e in range(each):
            for k in range(freqs):
                total = weights[k, 0] * times[u, 0, e]
                for s in range(1, groups):
                    total += weights[k, s] * times[u, s, e]
                out[k, u * each + e] = total

    early = 0
    phases = -(-count // cap)
    for phase in range(phases):
        @pl.loop(phase * cap, min(count, (phase + 1) * cap), unroll=16)
        def _(s):
            product(s)

        for rank in range(phase, phase + 1 if phase < phases - 1 else owners):
            ready(rank)
        upto = early
        if 1 <= phase < phases - 1:
            upto = early + 2 * phase

            @pl.loop(early, upto)
            def _(i):
                y_stage(i)
        early = upto

    items = nz * units
    passing = items - units
    hold, lag = 2, 3
    last = early + owners * lead

    @pl.loop(early, items + lag + hold)
    def _(t):
        @pl.when(t < items)
        def _():
            y_stage(t)

        @pl.when(t < last)
        def _():
            lead_stage(t - early)

        @pl.when(t == last)
        def _():
            @pl.loop(0, units)
            def _(u):
                y_copy(z, u).start()

        @pl.when(t < passing + early)
        def _():
            z_stage(t - early)

        @pl.when((t >= passing + lag) & (t < items + lag))
        def _():
            z_stage(t - lag)

        @pl.when((t >= passing + early) & (t < passing + early + lead))
        def _():
            cross_stage(t - passing - early)

        @pl.when((t >= passing + early + hold) & (t < passing + early + hold + lead))
        def _():
            out_stage(t - passing - early - hold + units)

        @pl.when(t >= passing + lag + hold)
        def _():
            out_stage(t - passing - lag - hold)

    @pl.loop(0, units)
    def _(u):
        @pl.loop(0, nz)
        def _(d):
            y_copy(d, u).wait_send()

            @pl.when(d > z)
            def _():
                z_copy(True, d, u, y_in.at[d, u]).wait_send()

            @pl.when(d < z)
            def _():
                z_copy(False, d, u, y_in.at[d, u]).wait_send()

        for step in range(1, groups):
            swap(y_in.at[z, u], u, step).wait_send()

    @pl.loop(0, lead)
    def _(w):
        @pl.loop(0, nz)
        def _(d):
            for yy in range(ny):
                @pl.when(d > z)
                def _():
                    z2_copy(True, d, yy, w, lead_own.at[w, d, yy]).wait_send()

                @pl.when(d < z)
                def _():
                    z2_copy(False, d, yy, w, lead_own.at[w, d, yy]).wait_send()

        y2_copy(w).wait_send()
        for step in range(1, groups):
            swap(lead_own.at[w, z, y], units + w, step).wait_send()


def slot_tables(target, nz, span):
    ny = 2
    tile = lax.axis_index("tile")
    z, y = tile // ny, tile % ny
    owner = target // span
    zd, yd = owner // ny, owner % ny
    rank = (yd == y).astype(jnp.int32)
    for k in range(nz):
        rank += jnp.where(zd == far_first(nz, z, k), 2 * k, 0)
    key = rank * span + target % span
    p = jnp.arange(key.shape[0], dtype=jnp.int32)
    before = (key[None, :] < key[:, None]) | ((key[None, :] == key[:, None]) & (p[None, :] < p[:, None]))
    position = jnp.sum(before.astype(jnp.int32), axis=1)
    again = jnp.any((key[None, :] == key[:, None]) & (p[None, :] < p[:, None]), axis=1)
    code = 2 * p + again.astype(jnp.int32)
    order = jnp.sum(jnp.where(position[None, :] == p[:, None], code[None, :], 0), axis=1)
    place = jnp.arange(nz * ny * span, dtype=jnp.int32)
    big = 2 * key.shape[0]
    found = jnp.sum((key[None, :] <= place[:, None]).astype(jnp.int32)
                    + jnp.where(key[None, :] == place[:, None], big, 0), axis=1)
    return order, jnp.where(found >= big, found % big, 0)


def fused(occ, virt, weights, occ_idx, virt_idx, target, nz, groups):
    count, terms = occ_idx.shape
    size = occ.shape[1]
    ny, span = 2, CHI_DEV
    each = UNIT
    lead = max(1, int(span // each * Z_FIRST))
    units = span // each - lead
    rows = size // groups
    block = (groups, each, rows, size)
    freqs = weights.shape[0]
    order, slot = slot_tables(target, nz, span)
    smem = pl.BlockSpec(memory_space=pltpu.SMEM)
    vmem = pl.BlockSpec(memory_space=pltpu.VMEM)
    dma = pltpu.SemaphoreType.DMA
    f32 = jnp.float32
    return pl.pallas_call(
        functools.partial(fused_kernel, nz, groups, terms, 2 * count // (nz * ny)),
        out_shape=pltpu.VMEM((freqs, span, rows, size), f32),
        in_specs=[smem] * 5 + [pl.BlockSpec(memory_space=pl.ANY)] * 2,
        out_specs=vmem,
        scratch_shapes=[
            pltpu.VMEM(occ.shape, occ.dtype),
            pltpu.VMEM(virt.shape, virt.dtype),
            dma((2,)),
            pltpu.VMEM((count + 1, size, size), f32),
            pltpu.VMEM((nz, units) + block, f32),
            pltpu.VMEM((nz, units) + block, f32),
            pltpu.VMEM((nz - 1, units) + block, f32),
            pltpu.VMEM((nz - 1, units) + block, f32),
            pltpu.VMEM((lead, nz, ny) + block, f32),
            pltpu.VMEM((nz - 1, ny, lead) + block, f32),
            pltpu.VMEM((nz - 1, ny, lead) + block, f32),
            pltpu.VMEM((lead,) + block, f32),
            pltpu.VMEM((units + lead,) + block, f32),
            dma((nz * units,)),
            dma((nz * units,)),
            dma((nz * units,)),
            dma(((nz - 1) * units,)),
            dma(((nz - 1) * units,)),
            dma((nz * ny * lead,)),
            dma(((nz - 1) * ny * lead,)),
            dma(((nz - 1) * ny * lead,)),
            dma((lead,)),
            dma((lead,)),
            dma(((units + lead) * groups,)),
            dma(((units + lead) * groups,)),
        ],
        compiler_params=pltpu.CompilerParams(
            collective_id=0, has_side_effects=True, vmem_limit_bytes=57 * 1024 * 1024),
    )(weights, order, slot, occ_idx.T, virt_idx.T, occ, virt)


def body(occupied, virtual, cos_weights, pair_occ, pair_virt, partial_target_tile):
    owners = lax.axis_size("tile")
    groups = lax.axis_size("tau")
    size = occupied.shape[2]
    ny = 1
    while 2 * ny * 2 * ny <= owners:
        ny *= 2
    nz = owners // ny
    if ny == 2 and nz == 4:
        return fused(occupied[0], virtual[0], cos_weights, pair_occ, pair_virt,
                     partial_target_tile, nz, groups)
    tile_bytes = 4 * size * size
    span = CHI_DEV
    while span > UNIT and span * tile_bytes * (
        nz * (1 + line_slots(ny)) + line_slots(nz) + 2
    ) > BUDGET:
        span //= 2
    results = []
    for q in range(CHI_DEV // span):
        dense = products(
            occupied[0], virtual[0], pair_occ, pair_virt, partial_target_tile,
            q * span, span, min(UNIT, span), owners, groups,
        )
        results.append(scatter(dense, cos_weights, ny, nz, groups))
    return results[0] if len(results) == 1 else jnp.concatenate(results, axis=1)


def solution(mesh):
    in_specs = (
        P("tau", "tile", None, None),
        P("tau", "tile", None, None),
        P(),
        P("tile", None),
        P("tile", None),
        P("tile"),
    )
    out_specs = P(None, "tile", "tau", None)
    return jax.shard_map(body, mesh=mesh, in_specs=in_specs, out_specs=out_specs, check_vma=False)
```

```python
import functools
import math

import jax
import jax.numpy as jnp
from jax import lax
from jax.experimental import pallas as pl
from jax.experimental.pallas import tpu as pltpu
from jax.sharding import PartitionSpec as P

CHI_DEV = 32
UNIT = 2
Z_FIRST = 3 / 16
BUDGET = 46 * 1024 * 1024
MESH = pl.DeviceIdType.MESH


def products_kernel(first, terms, chi_dev, occ_idx, virt_idx, target, occ, virt, out):
    owners, units, groups, each, rows, width = out.shape
    span = units * each
    count = target.shape[0]

    @pl.loop(0, owners)
    def _(d):
        out[d] = jnp.zeros(out.shape[1:], out.dtype)

    unroll = math.gcd(count, 4) if span == chi_dev else 1

    @pl.loop(0, count, unroll=unroll)
    def _(p):
        tile = target[p]
        owner = tile // chi_dev
        place = tile - owner * chi_dev - first

        def add():
            unit = place // each
            left = [occ[occ_idx[j, p]] for j in range(terms)]
            right = [virt[virt_idx[j, p]] for j in range(terms)]
            acc = jnp.dot(
                jnp.concatenate(left, axis=1),
                jnp.concatenate(right, axis=0),
                preferred_element_type=jnp.float32,
            )
            for g in range(groups):
                out[owner, unit, g, place - unit * each] += acc[g * rows : (g + 1) * rows]

        if span == chi_dev:
            add()
        else:
            pl.when((place >= 0) & (place < span))(add)


def products(occ, virt, occ_idx, virt_idx, target, first, span, each, owners, groups):
    terms = occ_idx.shape[1]
    size = occ.shape[1]
    smem = pl.BlockSpec(memory_space=pltpu.SMEM)
    vmem = pl.BlockSpec(memory_space=pltpu.VMEM)
    return pl.pallas_call(
        functools.partial(products_kernel, first, terms, CHI_DEV),
        out_shape=jax.ShapeDtypeStruct(
            (owners, span // each, groups, each, size // groups, size), jnp.float32
        ),
        in_specs=[smem, smem, smem, vmem, vmem],
        out_specs=vmem,
        compiler_params=pltpu.CompilerParams(vmem_limit_bytes=56 * 1024 * 1024),
        cost_estimate=pl.CostEstimate(
            flops=2 * target.shape[0] * terms * size**3 * span // CHI_DEV,
            bytes_accessed=occ.size * 4 + owners * span * size * size * 4,
            transcendentals=0,
        ),
    )(occ_idx.T, virt_idx.T, target, occ, virt)


def line_slots(n):
    if n == 1:
        return 0
    return 1 if n == 2 else 2 * (n - 1)


class Line:
    def __init__(self, n, place, device, own, slots, send_sem, recv_sem, hold=None):
        self.hold = hold
        self.n, self.place, self.device = n, place, device
        self.own, self.slots, self.send_sem, self.recv_sem = own, slots, send_sem, recv_sem

    def slot(self, right, d):
        if right:
            return d - 1
        return d if self.n == 2 else self.n - 1 + d

    def copy(self, right, u, d, src, back=False):
        s = self.slot(right, d)
        k = u * line_slots(self.n) + s
        return pltpu.make_async_remote_copy(
            src_ref=src,
            dst_ref=self.slots.at[s, u],
            send_sem=self.send_sem.at[k],
            recv_sem=self.recv_sem.at[k],
            device_id={"tile": self.device(1 if right != back else -1)},
            device_id_type=MESH,
        )

    def routes(self):
        for right in (True, False):
            for d in range(self.n - 1, 0, -1) if right else range(self.n - 1):
                yield right, d

    def launch(self, u):
        for right, d in self.routes():
            @pl.when(self.place == (0 if right else self.n - 1))
            def _():
                self.copy(right, u, d, self.own(d, u)).start()

    def merge(self, u):
        if self.n == 2:
            return
        for right, d in self.routes():
            inner = (self.place > 0) & (self.place < d) if right else (
                (self.place < self.n - 1) & (self.place > d))

            @pl.when(inner)
            def _():
                here = self.slots.at[self.slot(right, d), u]
                copy = self.copy(right, u, d, here)
                copy.wait_recv()
                own = self.own(d, u)
                if self.hold is not None:
                    buffer, sem = self.hold
                    fetch = pltpu.make_async_copy(own, buffer, sem)
                    fetch.start()
                    fetch.wait()
                    own = buffer
                here[...] += own[...]
                copy.start()

    def final(self, u, into):
        for right in (True, False):
            @pl.when(self.place > 0 if right else self.place < self.n - 1)
            def _():
                k = self.slot(right, self.place)
                here = self.slots.at[k, u]
                self.copy(right, u, self.place, here, back=True).wait_recv()
                into[...] += here[...]

    def drain(self, u):
        for right, d in self.routes():
            @pl.when(self.place < d if right else self.place > d)
            def _():
                self.copy(right, u, d, self.slots.at[self.slot(right, d), u]).wait_send()


def scatter_kernel(ny, nz, groups, weights, dense, out, mine, y_slots, z_slots, times,
                   load_sem, y_send, y_recv, z_send, z_recv, t_send, t_recv, hold, hold_sem,
                   both, z2_slots, y2_slots, both_sem, z2_send, z2_recv, y2_send, y2_recv):
    tau = lax.axis_index("tau")
    tile = lax.axis_index("tile")
    z, y = tile // ny, tile % ny
    units = mine.shape[0]
    lead = both.shape[0]
    last = units - lead
    each = mine.shape[3]
    freqs = out.shape[0]

    y_line = Line(ny, y, lambda step: tile + step, lambda d, u: dense.at[:, d, u],
                  y_slots, y_send, y_recv, (hold, hold_sem))
    z_line = Line(nz, z, lambda step: tile + step * ny, lambda d, u: mine.at[u, d],
                  z_slots, z_send, z_recv)

    z2_line = Line(nz, z, z_line.device, lambda d, u: both.at[u, d], z2_slots, z2_send, z2_recv)
    y2_line = Line(ny, y, y_line.device, lambda d, u: both.at[u, z, d], y2_slots, y2_send, y2_recv)

    barrier = pltpu.get_barrier_semaphore()
    for step in range(1, groups):
        pl.semaphore_signal(barrier, inc=1, device_id={"tau": (tau + step) % groups},
                            device_id_type=MESH)
    for step in range(1, ny):
        pl.semaphore_signal(barrier, inc=1, device_id={"tile": z * ny + (y + step) % ny},
                            device_id_type=MESH)
    for step in range(1, nz):
        pl.semaphore_signal(barrier, inc=1, device_id={"tile": (z + step) % nz * ny + y},
                            device_id_type=MESH)
    pl.semaphore_wait(barrier, groups - 1 + ny - 1 + nz - 1)

    def load(u):
        return pltpu.make_async_copy(dense.at[:, y, u], mine.at[u], load_sem.at[u])

    def swap(u, step):
        other = (tau + step) % groups
        return pltpu.make_async_remote_copy(
            src_ref=mine.at[u, z, other],
            dst_ref=times.at[u, tau],
            send_sem=t_send.at[u * groups + step],
            recv_sem=t_recv.at[u * groups + tau],
            device_id={"tau": other},
            device_id_type=MESH,
        )

    def arrived(u, source):
        return pltpu.make_async_remote_copy(
            src_ref=mine.at[u, z, 0],
            dst_ref=times.at[u, source],
            send_sem=t_send.at[u * groups],
            recv_sem=t_recv.at[u * groups + source],
            device_id={"tau": source},
            device_id_type=MESH,
        )

    def whole(w):
        return pltpu.make_async_copy(dense.at[:, :, last + w], both.at[w], both_sem.at[w])

    @pl.loop(0, lead)
    def _(w):
        whole(w).start()

    @pl.loop(0, last)
    def _(u):
        y_line.launch(u)
        load(u).start()

    @pl.loop(0, lead)
    def _(w):
        whole(w).wait()
        z2_line.launch(w)

    @pl.loop(0, lead)
    def _(w):
        z2_line.merge(w)

    @pl.loop(0, units + 2)
    def _(t):
        @pl.when(t < last)
        def _():
            load(t).wait()
            y_line.merge(t)
            y_line.final(t, mine.at[t])
            z_line.launch(t)

        @pl.when(t < lead)
        def _():
            z2_line.final(t, both.at[t, z])
            y2_line.launch(t)

        @pl.when((t >= 1) & (t < last + 1))
        def _():
            u = t - 1
            z_line.merge(u)
            z_line.final(u, mine.at[u, z])

        @pl.when((t >= last + 1) & (t < units + 1))
        def _():
            w = t - 1 - last
            y2_line.merge(w)
            mine[t - 1, z] = both[w, z, y]
            y2_line.final(w, mine.at[t - 1, z])

        @pl.when((t >= 1) & (t < units + 1))
        def _():
            u = t - 1
            for step in range(1, groups):
                swap(u, step).start()
            times[u, tau] = mine[u, z, tau]

        @pl.when(t >= 2)
        def _():
            u = t - 2
            for step in range(1, groups):
                arrived(u, (tau + step) % groups).wait_recv()
            for e in range(each):
                for k in range(freqs):
                    total = weights[k, 0] * times[u, 0, e]
                    for s in range(1, groups):
                        total += weights[k, s] * times[u, s, e]
                    out[k, u * each + e] = total

    @pl.loop(0, lead)
    def _(w):
        z2_line.drain(w)
        y2_line.drain(w)

    @pl.loop(0, last)
    def _(u):
        y_line.drain(u)
        z_line.drain(u)

    @pl.loop(0, units)
    def _(u):
        for step in range(1, groups):
            swap(u, step).wait_send()


def scatter(dense, weights, ny, nz, groups):
    owners, units, _, each, rows, width = dense.shape
    freqs = weights.shape[0]
    block = (groups, each, rows, width)
    lead = max(1, int(units * Z_FIRST))
    ys, zs = max(line_slots(ny), 1), max(line_slots(nz), 1)
    dma = pltpu.SemaphoreType.DMA
    return pl.pallas_call(
        functools.partial(scatter_kernel, ny, nz, groups),
        out_shape=jax.ShapeDtypeStruct((freqs, units * each, rows, width), jnp.float32),
        in_specs=[pl.BlockSpec(memory_space=pltpu.SMEM), pl.BlockSpec(memory_space=pl.ANY)],
        out_specs=pl.BlockSpec(memory_space=pltpu.VMEM),
        scratch_shapes=[
            pltpu.VMEM((units, nz) + block, jnp.float32),
            pltpu.VMEM((ys, units, nz) + block, jnp.float32),
            pltpu.VMEM((zs, units) + block, jnp.float32),
            pltpu.VMEM((units, groups, each, rows, width), jnp.float32),
            dma((units,)),
            dma((units * ys,)),
            dma((units * ys,)),
            dma((units * zs,)),
            dma((units * zs,)),
            dma((units * groups,)),
            dma((units * groups,)),
            pltpu.VMEM((nz,) + block if ny > 2 else (8, 128), jnp.float32),
            dma,
            pltpu.VMEM((lead, nz, ny) + block, jnp.float32),
            pltpu.VMEM((zs, lead, ny) + block, jnp.float32),
            pltpu.VMEM((ys, lead) + block, jnp.float32),
            dma((lead,)),
            dma((lead * zs,)),
            dma((lead * zs,)),
            dma((lead * ys,)),
            dma((lead * ys,)),
        ],
        compiler_params=pltpu.CompilerParams(
            collective_id=0, has_side_effects=True, vmem_limit_bytes=58 * 1024 * 1024),
    )(weights, dense.reshape((nz, ny) + dense.shape[1:]))


def far_first(nz, z, k):
    flip = z // (nz // 2)
    m = z + flip * (nz - 1 - 2 * z)
    ends = nz - 1 - k
    inner = (1 - k % 2) * (nz - 1 - k // 2) + (k % 2) * (k // 2)
    e = (1 - m) * ends + m * inner
    return e + flip * (nz - 1 - 2 * e)


def fused_kernel(nz, groups, terms, cap, weights, order, slot, occ_idx, virt_idx, occ_hbm, virt_hbm,
                 out, occ, virt, load_sem, packed, y_out, y_in, z_right, z_left, lead_own, z2_right, z2_left, y2_in,
                 times, y_send, y_recv, z_send, zr_recv, zl_recv, z2_send, z2r_recv, z2l_recv,
                 y2_send, y2_recv, t_send, t_recv):
    tau = lax.axis_index("tau")
    tile = lax.axis_index("tile")
    ny = 2
    z, y = tile // ny, tile % ny
    other_y = 1 - y
    lead = lead_own.shape[0]
    units = y_out.shape[1]
    each, rows = y_out.shape[3], y_out.shape[4]
    span = (units + lead) * each
    owners = nz * ny
    count = order.shape[0]
    freqs = out.shape[0]

    def dest(k):
        return far_first(nz, z, k)

    def remote(src, dst, send, recv, device):
        return pltpu.make_async_remote_copy(
            src_ref=src, dst_ref=dst, send_sem=send, recv_sem=recv,
            device_id=device, device_id_type=MESH)

    def y_copy(d, u):
        k = d * units + u
        return remote(y_out.at[d, u], y_in.at[d, u], y_send.at[k], y_recv.at[k],
                      {"tile": z * ny + other_y})

    def z_copy(right, d, u, src, back=False):
        if right:
            k = (d - 1) * units + u
            dst, recv = z_right.at[d - 1, u], zr_recv.at[k]
        else:
            k = d * units + u
            dst, recv = z_left.at[d, u], zl_recv.at[k]
        return remote(src, dst, z_send.at[d * units + u], recv,
                      {"tile": tile + (ny if right != back else -ny)})

    def z2_copy(right, d, yy, w, src, back=False):
        k = (d * ny + yy) * lead + w
        if right:
            dst, recv = z2_right.at[d - 1, yy, w], z2r_recv.at[k - ny * lead]
        else:
            dst, recv = z2_left.at[d, yy, w], z2l_recv.at[k]
        return remote(src, dst, z2_send.at[k], recv,
                      {"tile": tile + (ny if right != back else -ny)})

    def y2_copy(w):
        return remote(lead_own.at[w, z, other_y], y2_in.at[w], y2_send.at[w], y2_recv.at[w],
                      {"tile": z * ny + other_y})

    def swap(src, u, step):
        other = (tau + step) % groups
        return remote(src.at[other], times.at[u, tau], t_send.at[u * groups + step],
                      t_recv.at[u * groups + tau], {"tau": other})

    def arrived(u, source):
        return remote(times.at[u, tau], times.at[u, source], t_send.at[u * groups],
                      t_recv.at[u * groups + source], {"tau": source})

    loads = [pltpu.make_async_copy(occ_hbm, occ, load_sem.at[0]),
             pltpu.make_async_copy(virt_hbm, virt, load_sem.at[1])]
    for load in loads:
        load.start()

    barrier = pltpu.get_barrier_semaphore()
    for step in range(1, groups):
        pl.semaphore_signal(barrier, inc=1, device_id={"tau": (tau + step) % groups},
                            device_id_type=MESH)
    pl.semaphore_signal(barrier, inc=1, device_id={"tile": z * ny + other_y}, device_id_type=MESH)
    @pl.when(z > 0)
    def _():
        pl.semaphore_signal(barrier, inc=1, device_id={"tile": tile - ny}, device_id_type=MESH)

    @pl.when(z < nz - 1)
    def _():
        pl.semaphore_signal(barrier, inc=1, device_id={"tile": tile + ny}, device_id_type=MESH)

    beside = (z + nz - 1) // nz + (2 * nz - 2 - z) // nz
    pl.semaphore_wait(barrier, groups - 1 + ny - 1 + beside)

    packed[0] = jnp.zeros(packed.shape[1:], packed.dtype)
    for load in loads:
        load.wait()

    def product(s):
        p = order[s] // 2
        keep = (order[s] % 2).astype(jnp.float32)
        left = [occ[occ_idx[j, p]] for j in range(terms)]
        right = [virt[virt_idx[j, p]] for j in range(terms)]
        acc = jnp.dot(
            jnp.concatenate(left, axis=1),
            jnp.concatenate(right, axis=0),
            preferred_element_type=jnp.float32,
        )
        packed[s + 1] = acc + keep * packed[s]

    def fill(rank, u, ref, add):
        for e in range(each):
            part = packed[slot[rank * span + u * each + e]]
            for g in range(groups):
                piece = part[g * rows:(g + 1) * rows]
                if add:
                    ref[g, e] += piece
                else:
                    ref[g, e] = piece

    def ready(rank):
        d = dest(rank // 2)
        yy = y if rank % 2 else other_y
        @pl.loop(0, lead)
        def _(w):
            own = lead_own.at[w, d, yy]
            fill(rank, units + w, own, False)

            @pl.when((z == 0) & (d > z))
            def _():
                z2_copy(True, d, yy, w, own).start()

            @pl.when((z == nz - 1) & (d < z))
            def _():
                z2_copy(False, d, yy, w, own).start()

        if rank % 2 == 0:
            @pl.loop(0, units)
            def _(u):
                fill(rank, u, y_out.at[d, u], False)
                if rank < owners - ny:
                    y_copy(d, u).start()

    def y_stage(i):
        k, u = i // units, i % units
        d = dest(k)
        here = y_in.at[d, u]
        y_copy(d, u).wait_recv()
        fill(2 * k + 1, u, here, True)

        @pl.when((z == 0) & (d > z))
        def _():
            z_copy(True, d, u, here).start()

        @pl.when((z == nz - 1) & (d < z))
        def _():
            z_copy(False, d, u, here).start()

    def z_sent(d, u):
        @pl.when(d > z)
        def _():
            z_copy(True, d, u, y_in.at[d, u]).wait_send()

        @pl.when(d < z)
        def _():
            z_copy(False, d, u, y_in.at[d, u]).wait_send()

    def z_stage(i):
        k, u = i // units, i % units
        d = dest(k)
        own = y_in.at[d, u]

        @pl.when((z > 0) & (d > z))
        def _():
            here = z_right.at[d - 1, u]
            copy = z_copy(True, d, u, here)
            copy.wait_recv()
            here[...] += own[...]
            copy.start()

        @pl.when((z < nz - 1) & (d < z))
        def _():
            here = z_left.at[d, u]
            copy = z_copy(False, d, u, here)
            copy.wait_recv()
            here[...] += own[...]
            copy.start()

        @pl.when((d == z) & (z > 0))
        def _():
            here = z_right.at[z - 1, u]
            z_copy(True, z, u, here, True).wait_recv()
            own[...] += here[...]

        @pl.when((d == z) & (z < nz - 1))
        def _():
            here = z_left.at[z, u]
            z_copy(False, z, u, here, True).wait_recv()
            own[...] += here[...]

        @pl.when(d == z)
        def _():
            for step in range(1, groups):
                swap(own, u, step).start()
            times[u, tau] = own[tau]

    def lead_stage(j):
        rank, w = j // lead, j % lead
        d = dest(rank // 2)
        yy = y + (1 - rank % 2) * (1 - 2 * y)
        own = lead_own.at[w, d, yy]

        @pl.when((z > 0) & (d > z))
        def _():
            here = z2_right.at[d - 1, yy, w]
            copy = z2_copy(True, d, yy, w, here)
            copy.wait_recv()
            here[...] += own[...]
            copy.start()

        @pl.when((z < nz - 1) & (d < z))
        def _():
            here = z2_left.at[d, yy, w]
            copy = z2_copy(False, d, yy, w, here)
            copy.wait_recv()
            here[...] += own[...]
            copy.start()

        @pl.when((d == z) & (z > 0))
        def _():
            here = z2_right.at[z - 1, yy, w]
            z2_copy(True, z, yy, w, here, True).wait_recv()
            own[...] += here[...]

        @pl.when((d == z) & (z < nz - 1))
        def _():
            here = z2_left.at[z, yy, w]
            z2_copy(False, z, yy, w, here, True).wait_recv()
            own[...] += here[...]

        @pl.when((d == z) & (rank % 2 == 0))
        def _():
            y2_copy(w).start()

    def cross_stage(w):
        own = lead_own.at[w, z, y]
        y2_copy(w).wait_recv()
        own[...] += y2_in[w]
        for step in range(1, groups):
            swap(own, units + w, step).start()
        times[units + w, tau] = own[tau]

    def out_stage(u):
        for step in range(1, groups):
            arrived(u, (tau + step) % groups).wait_recv()
        for e in range(each):
            for k in range(freqs):
                total = weights[k, 0] * times[u, 0, e]
                for s in range(1, groups):
                    total += weights[k, s] * times[u, s, e]
                out[k, u * each + e] = total

    early = 0
    phases = -(-count // cap)
    for phase in range(phases):
        @pl.loop(phase * cap, min(count, (phase + 1) * cap), unroll=16)
        def _(s):
            product(s)

        for rank in range(phase, phase + 1 if phase < phases - 1 else owners):
            ready(rank)
        upto = early
        if 1 <= phase < phases - 1:
            upto = early + 2 * phase

            @pl.loop(early, upto)
            def _(i):
                y_stage(i)
        early = upto

    items = nz * units
    passing = items - units
    hold, lag = 2, 3
    last = early + owners * lead

    @pl.loop(early, items + lag + hold)
    def _(t):
        @pl.when(t < items)
        def _():
            y_stage(t)

        @pl.when(t < last)
        def _():
            lead_stage(t - early)

        @pl.when(t == last)
        def _():
            @pl.loop(0, units)
            def _(u):
                y_copy(z, u).start()

        @pl.when(t < passing + early)
        def _():
            z_stage(t - early)

        @pl.when((t >= passing + lag) & (t < items + lag))
        def _():
            z_stage(t - lag)

        @pl.when((t >= passing + early) & (t < passing + early + lead))
        def _():
            cross_stage(t - passing - early)

        @pl.when((t >= passing + early + hold) & (t < passing + early + hold + lead))
        def _():
            out_stage(t - passing - early - hold + units)

        @pl.when(t >= passing + lag + hold)
        def _():
            out_stage(t - passing - lag - hold)

        @pl.when((t >= passing + lag) & (t < items + lag))
        def _():
            u = t - passing - lag
            for k in range(nz - 1):
                y_copy(dest(k), u).wait_send()
            for k in range(nz - 2):
                z_sent(dest(k), u)

    @pl.loop(0, units)
    def _(u):
        y_copy(z, u).wait_send()
        z_sent(dest(nz - 2), u)
        for step in range(1, groups):
            swap(y_in.at[z, u], u, step).wait_send()

    @pl.loop(0, lead)
    def _(w):
        @pl.loop(0, nz)
        def _(d):
            for yy in range(ny):
                @pl.when(d > z)
                def _():
                    z2_copy(True, d, yy, w, lead_own.at[w, d, yy]).wait_send()

                @pl.when(d < z)
                def _():
                    z2_copy(False, d, yy, w, lead_own.at[w, d, yy]).wait_send()

        y2_copy(w).wait_send()
        for step in range(1, groups):
            swap(lead_own.at[w, z, y], units + w, step).wait_send()


def slot_tables(target, nz, span):
    ny = 2
    tile = lax.axis_index("tile")
    z, y = tile // ny, tile % ny
    owner = target // span
    zd, yd = owner // ny, owner % ny
    rank = (yd == y).astype(jnp.int32)
    for k in range(nz):
        rank += jnp.where(zd == far_first(nz, z, k), 2 * k, 0)
    key = rank * span + target % span
    p = jnp.arange(key.shape[0], dtype=jnp.int32)
    before = (key[None, :] < key[:, None]) | ((key[None, :] == key[:, None]) & (p[None, :] < p[:, None]))
    position = jnp.sum(before.astype(jnp.int32), axis=1)
    again = jnp.any((key[None, :] == key[:, None]) & (p[None, :] < p[:, None]), axis=1)
    code = 2 * p + again.astype(jnp.int32)
    order = jnp.sum(jnp.where(position[None, :] == p[:, None], code[None, :], 0), axis=1)
    place = jnp.arange(nz * ny * span, dtype=jnp.int32)
    big = 2 * key.shape[0]
    found = jnp.sum((key[None, :] <= place[:, None]).astype(jnp.int32)
                    + jnp.where(key[None, :] == place[:, None], big, 0), axis=1)
    return order, jnp.where(found >= big, found % big, 0)


def fused(occ, virt, weights, occ_idx, virt_idx, target, nz, groups):
    count, terms = occ_idx.shape
    size = occ.shape[1]
    ny, span = 2, CHI_DEV
    each = UNIT
    lead = max(1, int(span // each * Z_FIRST))
    units = span // each - lead
    rows = size // groups
    block = (groups, each, rows, size)
    freqs = weights.shape[0]
    order, slot = slot_tables(target, nz, span)
    smem = pl.BlockSpec(memory_space=pltpu.SMEM)
    vmem = pl.BlockSpec(memory_space=pltpu.VMEM)
    dma = pltpu.SemaphoreType.DMA
    f32 = jnp.float32
    return pl.pallas_call(
        functools.partial(fused_kernel, nz, groups, terms, 2 * count // (nz * ny)),
        out_shape=pltpu.VMEM((freqs, span, rows, size), f32),
        in_specs=[smem] * 5 + [pl.BlockSpec(memory_space=pl.ANY)] * 2,
        out_specs=vmem,
        scratch_shapes=[
            pltpu.VMEM(occ.shape, occ.dtype),
            pltpu.VMEM(virt.shape, virt.dtype),
            dma((2,)),
            pltpu.VMEM((count + 1, size, size), f32),
            pltpu.VMEM((nz, units) + block, f32),
            pltpu.VMEM((nz, units) + block, f32),
            pltpu.VMEM((nz - 1, units) + block, f32),
            pltpu.VMEM((nz - 1, units) + block, f32),
            pltpu.VMEM((lead, nz, ny) + block, f32),
            pltpu.VMEM((nz - 1, ny, lead) + block, f32),
            pltpu.VMEM((nz - 1, ny, lead) + block, f32),
            pltpu.VMEM((lead,) + block, f32),
            pltpu.VMEM((units + lead,) + block, f32),
            dma((nz * units,)),
            dma((nz * units,)),
            dma((nz * units,)),
            dma(((nz - 1) * units,)),
            dma(((nz - 1) * units,)),
            dma((nz * ny * lead,)),
            dma(((nz - 1) * ny * lead,)),
            dma(((nz - 1) * ny * lead,)),
            dma((lead,)),
            dma((lead,)),
            dma(((units + lead) * groups,)),
            dma(((units + lead) * groups,)),
        ],
        compiler_params=pltpu.CompilerParams(
            collective_id=0, has_side_effects=True, vmem_limit_bytes=57 * 1024 * 1024),
    )(weights, order, slot, occ_idx.T, virt_idx.T, occ, virt)


def body(occupied, virtual, cos_weights, pair_occ, pair_virt, partial_target_tile):
    owners = lax.axis_size("tile")
    groups = lax.axis_size("tau")
    size = occupied.shape[2]
    ny = 1
    while 2 * ny * 2 * ny <= owners:
        ny *= 2
    nz = owners // ny
    if ny == 2 and nz == 4:
        return fused(occupied[0], virtual[0], cos_weights, pair_occ, pair_virt,
                     partial_target_tile, nz, groups)
    tile_bytes = 4 * size * size
    span = CHI_DEV
    while span > UNIT and span * tile_bytes * (
        nz * (1 + line_slots(ny)) + line_slots(nz) + 2
    ) > BUDGET:
        span //= 2
    results = []
    for q in range(CHI_DEV // span):
        dense = products(
            occupied[0], virtual[0], pair_occ, pair_virt, partial_target_tile,
            q * span, span, min(UNIT, span), owners, groups,
        )
        results.append(scatter(dense, cos_weights, ny, nz, groups))
    return results[0] if len(results) == 1 else jnp.concatenate(results, axis=1)


def solution(mesh):
    in_specs = (
        P("tau", "tile", None, None),
        P("tau", "tile", None, None),
        P(),
        P("tile", None),
        P("tile", None),
        P("tile"),
    )
    out_specs = P(None, "tile", "tau", None)
    return jax.shard_map(body, mesh=mesh, in_specs=in_specs, out_specs=out_specs, check_vma=False)
```
